8 devices in a mesh: member: 1 (over z), lon: 2 (over y), lat: 4 (over x, core).
Axes of the slice: x: 2, y: 2, z: 1, core: 2. Of those that a mesh axis runs over, the one named last changes fastest.
Arguments:
- grid_field: float32 [4, 256, 256, 512], P('member', None, 'lat', 'lon')
- mix_weight: bfloat16 [256, 256, 256, 2], replicated
Outputs:
- output: float32 [4, 256, 256, 512], P('member', None, 'lat', 'lon')
All inputs are finite; a program needn't handle non-finite values.
Results may differ from the reference program's by a relative error of at most 0.00431334.
Values are sent between devices in bfloat16 or wider.
A program may use at most 1 GiB of HBM per device.

```python
import math
import jax
import jax.numpy as jnp
from jax import lax

BATCH_SIZE = 4
CHANNELS = 256
LAT_ROWS = 256
MAX_DEGREE = 256
LON_POINTS = 2 * LAT_ROWS


def legendre_table(m_vals, colatitude, n_deg):
    cos_t = jnp.cos(colatitude)[None, :]
    m_int = m_vals[:, None]
    m_col = m_int.astype(jnp.float32)
    deg_all = jnp.arange(1, n_deg + 1).astype(jnp.float32)
    log_steps = 0.5 * jnp.log((2.0 * deg_all + 1.0) / (2.0 * deg_all))
    cum_log = jnp.concatenate([jnp.zeros((1,), jnp.float32), jnp.cumsum(log_steps)])
    log_diag = 0.5 * math.log(0.5) + cum_log[m_vals][:, None] + m_col * jnp.log(jnp.sin(colatitude))[None, :]

    def degree_step(carry, degree):
        prev_one, prev_two, log_scale = carry
        deg_f = degree.astype(jnp.float32)
        at_start = m_int == degree
        is_above = m_int < degree
        coef_a = jnp.sqrt((4.0 * deg_f * deg_f - 1.0) / jnp.maximum(deg_f * deg_f - m_col * m_col, 1.0))
        coef_b = jnp.sqrt(jnp.maximum((deg_f - 1.0) ** 2 - m_col * m_col, 0.0) / jnp.maximum(4.0 * (deg_f - 1.0) ** 2 - 1.0, 1.0))
        rec_value = coef_a * (cos_t * prev_one - coef_b * prev_two)
        renorm = jnp.maximum(jnp.abs(rec_value), 1.0)
        next_one = jnp.where(at_start, 1.0, jnp.where(is_above, rec_value / renorm, 0.0))
        next_two = jnp.where(is_above, prev_one / renorm, 0.0)
        next_scale = jnp.where(at_start, log_diag, jnp.where(is_above, log_scale + jnp.log(renorm), 0.0))
        out_value = jnp.where(at_start | is_above, next_one * jnp.exp(next_scale), 0.0)
        return (next_one, next_two, next_scale), out_value

    zero_state = jnp.zeros((m_vals.shape[0], colatitude.shape[0]), jnp.float32)
    return lax.scan(degree_step, (zero_state, zero_state, zero_state), jnp.arange(n_deg))[1]


def fejer_weights(colatitude, n_lat):
    harmonic = jnp.arange(1, n_lat // 2 + 1).astype(jnp.float32)
    series = jnp.cos(2.0 * colatitude[:, None] * harmonic[None, :]) / (4.0 * harmonic * harmonic - 1.0)
    return (2.0 / n_lat) * (1.0 - 2.0 * jnp.sum(series, axis=1))


def dft_tables(n_lon, n_deg):
    lon_index = jnp.arange(n_lon)
    deg_index = jnp.arange(n_deg)
    fwd_angle = ((lon_index[:, None] * deg_index[None, :]) % n_lon).astype(jnp.float32) * (2.0 * math.pi / n_lon)
    fwd_table = jnp.concatenate([jnp.cos(fwd_angle), -jnp.sin(fwd_angle)], axis=1).astype(jnp.bfloat16)
    inv_angle = ((deg_index[:, None] * lon_index[None, :]) % n_lon).astype(jnp.float32) * (2.0 * math.pi / n_lon)
    weight_m = jnp.where(deg_index == 0, 1.0, 2.0)[:, None]
    inv_table = jnp.concatenate([weight_m * jnp.cos(inv_angle), -weight_m * jnp.sin(inv_angle)], axis=0).astype(jnp.bfloat16)
    return fwd_table, inv_table


def setup_inputs(seed: int = 0, part: int = 0) -> dict:
    part_key = jax.random.fold_in(jax.random.key(seed), part)
    noise_key, smooth_key = jax.random.split(part_key)
    colatitude = (jnp.arange(LAT_ROWS).astype(jnp.float32) + 0.5) * (math.pi / LAT_ROWS)
    longitude = jnp.arange(LON_POINTS).astype(jnp.float32) * (2.0 * math.pi / LON_POINTS)
    sin_lat = jnp.sin(colatitude)[:, None]
    smooth_basis = jnp.stack([jnp.broadcast_to(jnp.cos(colatitude)[:, None], (LAT_ROWS, LON_POINTS)), sin_lat * jnp.cos(longitude)[None, :], sin_lat * jnp.sin(longitude)[None, :]])
    smooth_amp = jax.random.normal(smooth_key, (BATCH_SIZE, CHANNELS, 3), jnp.float32)
    noise_part = jax.random.normal(noise_key, (BATCH_SIZE, CHANNELS, LAT_ROWS, LON_POINTS), jnp.float32)
    grid_field = noise_part + jnp.einsum('bcs,skj->bckj', smooth_amp, smooth_basis)
    weight_key = jax.random.key(seed + 1)
    mix_weight = (jax.random.normal(weight_key, (MAX_DEGREE, CHANNELS, CHANNELS, 2), jnp.float32) * CHANNELS ** -0.5).astype(jnp.bfloat16)
    return {'grid_field': grid_field, 'mix_weight': mix_weight}


def reference(grid_field, mix_weight):
    fwd_table, inv_table = dft_tables(LON_POINTS, MAX_DEGREE)
    colatitude = (jnp.arange(LAT_ROWS).astype(jnp.float32) + 0.5) * (math.pi / LAT_ROWS)
    leg_table = legendre_table(jnp.arange(MAX_DEGREE), colatitude, MAX_DEGREE)
    leg_fwd = (leg_table * (fejer_weights(colatitude, LAT_ROWS) / LON_POINTS)).astype(jnp.bfloat16).astype(jnp.float32)
    leg_inv = leg_table.astype(jnp.bfloat16).astype(jnp.float32)
    weight_f = mix_weight.astype(jnp.float32)
    weight_re = weight_f[..., 0]
    weight_im = weight_f[..., 1]

    def layer_sample(sample_field):
        field_bf = sample_field.astype(jnp.bfloat16)
        fourier = jnp.dot(field_bf.reshape(CHANNELS * LAT_ROWS, LON_POINTS), fwd_table, preferred_element_type=jnp.float32)
        fourier = fourier.astype(jnp.bfloat16).astype(jnp.float32).reshape(CHANNELS, LAT_ROWS, 2, MAX_DEGREE)
        spec_coef = jnp.einsum('ckrm,lmk->clrm', fourier, leg_fwd).astype(jnp.bfloat16).astype(jnp.float32)
        coef_re = spec_coef[:, :, 0, :]
        coef_im = spec_coef[:, :, 1, :]
        mixed_re = jnp.einsum('ilm,lio->olm', coef_re, weight_re) - jnp.einsum('ilm,lio->olm', coef_im, weight_im)
        mixed_im = jnp.einsum('ilm,lio->olm', coef_im, weight_re) + jnp.einsum('ilm,lio->olm', coef_re, weight_im)
        mixed_coef = jnp.stack([mixed_re, mixed_im], axis=2).astype(jnp.bfloat16).astype(jnp.float32)
        spec_grid = jnp.einsum('clrm,lmk->ckrm', mixed_coef, leg_inv).astype(jnp.bfloat16)
        grid_out = jnp.dot(spec_grid.reshape(CHANNELS * LAT_ROWS, 2 * MAX_DEGREE), inv_table, preferred_element_type=jnp.float32)
        grid_out = grid_out.astype(jnp.bfloat16).astype(jnp.float32).reshape(CHANNELS, LAT_ROWS, LON_POINTS)
        return sample_field + jax.nn.gelu(grid_out, approximate=False)

    return lax.map(layer_sample, grid_field)
```

```python
import functools
import math
import numpy as np
import jax
import jax.numpy as jnp
from jax import lax
from jax.experimental import pallas as pl
from jax.experimental.pallas import tpu as pltpu
from jax.sharding import PartitionSpec as P


BF = jnp.bfloat16
F32 = jnp.float32
LB = 16
NCHUNK = 4
MB = 8
NT = (((1,), (1,)), ((), ()))
TN = (((0,), (0,)), ((), ()))


def legendre_tables(n_lat, n_lon, n_deg):
    t = (np.arange(n_lat) + 0.5) * (math.pi / n_lat)
    x = np.cos(t)
    m = np.arange(n_deg)
    steps = np.concatenate([[0.0], np.cumsum(0.5 * np.log((2.0 * m[1:] + 1.0) / (2.0 * m[1:])))])
    diag = np.exp(0.5 * math.log(0.5) + steps[:, None] + m[:, None] * np.log(np.sin(t))[None, :])
    tab = np.zeros((n_deg, n_deg, n_lat))
    mm = m[:, None].astype(np.float64)
    prev1 = np.zeros((n_deg, n_lat))
    prev2 = np.zeros((n_deg, n_lat))
    for l in range(n_deg):
        a = np.sqrt((4.0 * l * l - 1.0) / np.maximum(l * l - mm * mm, 1.0)) if l > 0 else np.ones_like(mm)
        b = np.sqrt(np.maximum((l - 1.0) ** 2 - mm * mm, 0.0) / max(4.0 * (l - 1.0) ** 2 - 1.0, 1.0))
        cur = np.where(mm < l, a * (x[None, :] * prev1 - b * prev2), 0.0)
        cur[l] = diag[l]
        tab[:, l, :] = cur
        prev2 = prev1
        prev1 = cur
    n = np.arange(1, n_lat // 2 + 1)
    series = np.sum(np.cos(2.0 * t[:, None] * n[None, :]) / (4.0 * n * n - 1.0), axis=1)
    w = (2.0 / n_lat) * (1.0 - 2.0 * series)

    def pack(p):
        p = p.astype(np.float32).astype(BF).reshape(n_deg, n_deg // (2 * LB), 2, LB, n_lat)
        return np.ascontiguousarray(p.transpose(0, 2, 1, 3, 4)).reshape(n_deg, 2, n_deg // 2, n_lat)

    return pack(tab * (w / n_lon)), pack(tab)


def dft_tables(n_lon, n_deg):
    ang = ((np.arange(n_deg)[:, None] * np.arange(n_lon)[None, :]) % n_lon) * (2.0 * math.pi / n_lon)
    c_m = np.where(np.arange(n_deg) == 0, 1.0, 2.0)[:, None, None]
    fwd = np.stack([np.cos(ang), -np.sin(ang)], axis=1)

    def pack(p):
        p = p.astype(np.float32).astype(BF).reshape(2 * n_deg, 2, n_lon // 2)
        return np.ascontiguousarray(np.stack([p, p[:, ::-1]])).reshape(2, 2 * n_deg, n_lon)

    return pack(fwd), pack(c_m * fwd)


def cast_kernel(s_ref, *refs):
    n = len(refs) // 2
    for t in range(n):
        refs[n + t][...] = refs[t][0].astype(BF)


def fwd_dft_kernel(s_ref, tab_ref, *refs):
    pieces, out, scr, rc = refs[:8], refs[8], refs[9], refs[10]
    r = s_ref[2]
    rows = pieces[0].shape[1]
    cols = pieces[0].shape[2]
    nms = out.shape[0]

    def body(c, carry):
        for t in range(8):
            row = pl.multiple_of(((t & 3) ^ r) * rows, rows)
            q = t >> 2
            rc[pl.ds(row, rows), q * cols:(q + 1) * cols] = pieces[t][c]
        res = lax.dot_general(tab_ref[0], rc[...], NT, preferred_element_type=F32)
        for j in range(res.shape[1] // 128):
            scr[j, pl.ds(c, nms, stride=16), :] = res[:, j * 128:(j + 1) * 128]
        return carry

    lax.fori_loop(0, 16, body, 0)

    def flush(i, carry):
        for j in range(scr.shape[0]):
            blk = scr[j, pl.ds(pl.multiple_of(i * 512, 512), 512), :]
            out[pl.ds(i * 32, 32), :, j * 128:(j + 1) * 128] = blk.reshape(32, 16, 128).astype(BF)
        return carry

    lax.fori_loop(0, nms // 32, flush, 0)


def fwd_leg_kernel(s_ref, pw_ref, *refs):
    fs, out = refs[:-1], refs[-1]
    for m in range(MB):
        x = jnp.concatenate([f[2 * m + s] for s in range(2) for f in fs], axis=0)
        out[m] = lax.dot_general(pw_ref[m, 0], x, NT, preferred_element_type=F32).astype(BF)


def mix_kernel(s_ref, am, ar, wre, wim, bm, bs, scr_a, scr_b):
    h = s_ref[3]
    nm = am.shape[0]

    def fill(i, carry):
        rows = pl.ds(pl.multiple_of(i * 512, 512), 512)
        for sp in range(2):
            lanes = slice(sp * 128, sp * 128 + 128)
            scr_a[sp * 2 + h, rows, :] = am[pl.ds(i * 32, 32), :, lanes].astype(F32).reshape(512, 128)
            scr_a[sp * 2 + 1 - h, rows, :] = ar[pl.ds(i * 32, 32), :, lanes].astype(F32).reshape(512, 128)
        return carry

    lax.fori_loop(0, nm // 32, fill, 0)

    def body(li, carry):
        parts = [scr_a[b, pl.ds(li, nm, stride=LB), :].astype(BF) for b in range(4)]
        re = jnp.concatenate(parts[:2], axis=1)
        im = jnp.concatenate(parts[2:], axis=1)
        lhs = jnp.concatenate([re, im], axis=0)
        x = jnp.dot(lhs, wre[li], preferred_element_type=F32)
        y = jnp.dot(lhs, wim[li], preferred_element_type=F32)
        bre = x[:nm] - y[nm:]
        bim = x[nm:] + y[:nm]
        for b in range(2):
            scr_b[b, pl.ds(li, nm, stride=LB), :] = bre[:, b * 128:(b + 1) * 128]
            scr_b[2 + b, pl.ds(li, nm, stride=LB), :] = bim[:, b * 128:(b + 1) * 128]
        return carry

    lax.fori_loop(0, LB, body, 0)

    def flush(i, carry):
        rows = pl.ds(pl.multiple_of(i * 512, 512), 512)
        for sp in range(2):
            lanes = slice(sp * 128, sp * 128 + 128)
            bm[pl.ds(i * 32, 32), :, lanes] = scr_b[sp * 2 + h, rows, :].reshape(32, LB, 128).astype(BF)
            bs[pl.ds(i * 32, 32), :, lanes] = scr_b[sp * 2 + 1 - h, rows, :].reshape(32, LB, 128).astype(BF)
        return carry

    lax.fori_loop(0, nm // 32, flush, 0)


def inv_leg_kernel(s_ref, bm, br, pm_ref, pr_ref, *outs):
    n = outs[0].shape[1]
    for m in range(MB):
        b = jnp.concatenate([bm[m], br[m]], axis=0)
        p = jnp.concatenate([pm_ref[m, 0], pr_ref[m, 0]], axis=0)
        g = lax.dot_general(b, p, TN, preferred_element_type=F32).astype(BF)
        half = g.shape[0] // 2
        for s in range(2):
            for i, o in enumerate(outs):
                o[2 * m + s] = g[s * half + i * n:s * half + (i + 1) * n]


def inv_dft_kernel(s_ref, tab_ref, g_ref, *refs):
    pieces, scr, yc = refs[:8], refs[8], refs[9]
    r = s_ref[2]
    rows = pieces[0].shape[1]
    cols = pieces[0].shape[2]
    nms = g_ref.shape[0]

    def fill(i, carry):
        for j in range(scr.shape[0]):
            blk = g_ref[pl.ds(i * 32, 32), :, j * 128:(j + 1) * 128].astype(F32)
            scr[j, pl.ds(pl.multiple_of(i * 512, 512), 512), :] = blk.reshape(512, 128)
        return carry

    lax.fori_loop(0, nms // 32, fill, 0)

    def body(c, carry):
        g = jnp.concatenate([scr[j, pl.ds(c, nms, stride=16), :].astype(BF) for j in range(scr.shape[0])], axis=1)
        yc[...] = lax.dot_general(g, tab_ref[0], TN, preferred_element_type=F32).astype(BF)
        for t in range(8):
            row = pl.multiple_of(((t & 3) ^ r) * rows, rows)
            q = t >> 2
            pieces[t][c] = yc[pl.ds(row, rows), q * cols:(q + 1) * cols]
        return carry

    lax.fori_loop(0, 16, body, 0)


def call(kernel, grid, in_specs, out_specs, out_shape, flops, nbytes, scratch=()):
    return pl.pallas_call(
        kernel,
        grid_spec=pltpu.PrefetchScalarGridSpec(
            num_scalar_prefetch=1, grid=grid, in_specs=in_specs, out_specs=out_specs, scratch_shapes=list(scratch)),
        out_shape=out_shape,
        compiler_params=pltpu.CompilerParams(dimension_semantics=("arbitrary",) * len(grid), vmem_limit_bytes=56 * 2 ** 20),
        cost_estimate=pl.CostEstimate(flops=int(flops), bytes_accessed=int(nbytes), transcendentals=0),
    )


def solution(mesh):
    lat_devs = mesh.shape['lat']
    lon_devs = mesh.shape['lon']
    nd = lat_devs * lon_devs

    def local_layer(grid_field, mix_weight):
        batch, channels, row_count, col_count = grid_field.shape
        n_lat = row_count * lat_devs
        n_lon = col_count * lon_devs
        n_deg = mix_weight.shape[0]
        half_c = batch * channels // nd
        cc = half_c // NCHUNK
        nms = 2 * n_deg
        q = lax.axis_index('lon')
        r = lax.axis_index('lat')
        me = q * lat_devs + r
        h = r % 2
        scal = jnp.stack([me, q, r, h]).astype(jnp.int32)
        pw_np, pi_np = legendre_tables(n_lat, n_lon, n_deg)
        tf_np, ti_np = dft_tables(n_lon, n_deg)
        pw, pi, tf, ti = jnp.asarray(pw_np), jnp.asarray(pi_np), jnp.asarray(tf_np), jnp.asarray(ti_np)
        f8 = grid_field.reshape(nd, half_c, row_count, col_count)

        def swap(x, t):
            if t == 0:
                return x
            return lax.ppermute(x, ('lon', 'lat'), [(s, s ^ t) for s in range(nd)])

        piece = jax.ShapeDtypeStruct((cc, row_count, col_count), BF)
        tab_spec = pl.BlockSpec((1, nms, n_lon), lambda i, s: (s[1], 0, 0))
        piece_spec16 = pl.BlockSpec((16, row_count, col_count), lambda i, s: (i, 0, 0))

        def cast_chunk(k):
            cb = 8
            base = k * cc // cb
            return call(
                cast_kernel, (cc // cb,),
                [pl.BlockSpec((1, cb, row_count, col_count), functools.partial(lambda t, i, s: (s[0] ^ t, base + i, 0, 0), t)) for t in range(nd)],
                [pl.BlockSpec((cb, row_count, col_count), lambda i, s: (i, 0, 0))] * nd,
                [piece] * nd, 1e6, nd * cc * row_count * col_count * 6)(scal, *([f8] * nd))

        def dft_chunk(pieces):
            return call(
                fwd_dft_kernel, (cc // 16,),
                [tab_spec] + [piece_spec16] * nd,
                pl.BlockSpec((nms, 16, n_lat), lambda i, s: (0, i, 0)),
                jax.ShapeDtypeStruct((nms, cc, n_lat), BF),
                4.0 * cc * nms * n_lat * n_lon, cc * nms * n_lat * 6,
                [pltpu.VMEM((n_lat // 128, nms * 16, 128), F32), pltpu.VMEM((n_lat, n_lon), BF)])(scal, tf, *pieces)

        def leg_fwd(flag, fs):
            return call(
                fwd_leg_kernel, (n_deg // MB,),
                [pl.BlockSpec((MB, 1, n_deg // 2, n_lat), lambda i, s: (i, s[3] ^ flag, 0, 0))]
                + [pl.BlockSpec((2 * MB, cc, n_lat), lambda i, s: (i, 0, 0))] * NCHUNK,
                pl.BlockSpec((MB, n_deg // 2, 2 * half_c), lambda i, s: (i, 0, 0)),
                jax.ShapeDtypeStruct((n_deg, n_deg // 2, 2 * half_c), BF),
                2.0 * n_deg * n_deg * n_lat * half_c, 70e6)(scal, pw, *fs)

        recv = []
        for k in range(NCHUNK):
            pieces = cast_chunk(k)
            recv.append([swap(p, t) for t, p in enumerate(pieces)])
        fs = [dft_chunk(p) for p in recv]

        a_send = leg_fwd(1, fs)
        a_recv = swap(a_send, 1)
        a_mine = leg_fwd(0, fs)

        w = mix_weight.reshape(n_deg // (2 * LB), 2, LB, channels, channels, 2)
        w = lax.dynamic_index_in_dim(w, h, axis=1, keepdims=False).reshape(n_deg // 2, channels, channels, 2)
        w_re, w_im = w[..., 0], w[..., 1]

        a_spec = pl.BlockSpec((n_deg, LB, 2 * half_c), lambda i, s: (0, i, 0))
        w_spec = pl.BlockSpec((LB, channels, channels), lambda i, s: (i, 0, 0))
        spec_half = jax.ShapeDtypeStruct((n_deg, n_deg // 2, 2 * half_c), BF)
        b_mine, b_send = call(
            mix_kernel, (n_deg // 2 // LB,),
            [a_spec, a_spec, w_spec, w_spec], [a_spec, a_spec], [spec_half, spec_half],
            8.0 * n_deg * n_deg // 2 * channels * channels, 100e6,
            [pltpu.VMEM((4, n_deg * LB, 128), F32), pltpu.VMEM((4, n_deg * LB, 128), F32)])(scal, a_mine, a_recv, w_re, w_im)
        b_recv = swap(b_send, 1)

        b_spec = pl.BlockSpec((MB, n_deg // 2, 2 * half_c), lambda i, s: (i, 0, 0))
        gs = call(
            inv_leg_kernel, (n_deg // MB,),
            [b_spec, b_spec,
             pl.BlockSpec((MB, 1, n_deg // 2, n_lat), lambda i, s: (i, s[3], 0, 0)),
             pl.BlockSpec((MB, 1, n_deg // 2, n_lat), lambda i, s: (i, 1 - s[3], 0, 0))],
            [pl.BlockSpec((2 * MB, cc, n_lat), lambda i, s: (i, 0, 0))] * NCHUNK,
            [jax.ShapeDtypeStruct((nms, cc, n_lat), BF)] * NCHUNK,
            4.0 * n_deg * n_deg * n_lat * half_c, 100e6)(scal, b_mine, b_recv, pi, pi)

        def idft_chunk(g):
            return call(
                inv_dft_kernel, (cc // 16,),
                [tab_spec, pl.BlockSpec((nms, 16, n_lat), lambda i, s: (0, i, 0))],
                [piece_spec16] * nd, [piece] * nd,
                4.0 * cc * nms * n_lat * n_lon, cc * nms * n_lat * 6,
                [pltpu.VMEM((n_lat // 128, nms * 16, 128), F32), pltpu.VMEM((n_lat, n_lon), BF)])(scal, ti, g)

        out = jnp.zeros(f8.shape, F32)
        for k in range(NCHUNK):
            for t, p in enumerate(idft_chunk(gs[k])):
                y = swap(p, t).astype(F32)
                src = lax.dynamic_slice(f8, (me ^ t, k * cc, 0, 0), (1, cc, row_count, col_count))
                new = src + jax.nn.gelu(y, approximate=False)[None]
                out = lax.dynamic_update_slice(out, new, (me ^ t, k * cc, 0, 0))
        return out.reshape(grid_field.shape)

    field_spec = P('member', None, 'lat', 'lon')
    return jax.shard_map(local_layer, mesh=mesh, in_specs=(field_spec, P()), out_specs=field_spec, check_vma=False)
```

```python
import functools
import math
import numpy as np
import jax
import jax.numpy as jnp
from jax import lax
from jax.experimental import pallas as pl
from jax.experimental.pallas import tpu as pltpu
from jax.sharding import PartitionSpec as P


BF = jnp.bfloat16
F32 = jnp.float32
LB = 16
HALVES = ((16, 16, 32), (32, 16, 16))
MB = 16
MG = 64
NV = 4
NT = (((1,), (1,)), ((), ()))
TN = (((0,), (0,)), ((), ()))


def legendre_tables(n_lat, n_lon, n_deg):
    t = (np.arange(n_lat) + 0.5) * (math.pi / n_lat)
    x = np.cos(t)
    m = np.arange(n_deg)
    steps = np.concatenate([[0.0], np.cumsum(0.5 * np.log((2.0 * m[1:] + 1.0) / (2.0 * m[1:])))])
    diag = np.exp(0.5 * math.log(0.5) + steps[:, None] + m[:, None] * np.log(np.sin(t))[None, :])
    tab = np.zeros((n_deg, n_deg, n_lat))
    mm = m[:, None].astype(np.float64)
    prev1 = np.zeros((n_deg, n_lat))
    prev2 = np.zeros((n_deg, n_lat))
    for l in range(n_deg):
        a = np.sqrt((4.0 * l * l - 1.0) / np.maximum(l * l - mm * mm, 1.0)) if l > 0 else np.ones_like(mm)
        b = np.sqrt(np.maximum((l - 1.0) ** 2 - mm * mm, 0.0) / max(4.0 * (l - 1.0) ** 2 - 1.0, 1.0))
        cur = np.where(mm < l, a * (x[None, :] * prev1 - b * prev2), 0.0)
        cur[l] = diag[l]
        tab[:, l, :] = cur
        prev2 = prev1
        prev1 = cur
    n = np.arange(1, n_lat // 2 + 1)
    series = np.sum(np.cos(2.0 * t[:, None] * n[None, :]) / (4.0 * n * n - 1.0), axis=1)
    w = (2.0 / n_lat) * (1.0 - 2.0 * series)

    def pack(p):
        p = p.astype(np.float32).astype(BF).reshape(n_deg, n_deg // (2 * LB), 2, LB, n_lat)
        return np.ascontiguousarray(p.transpose(0, 2, 1, 3, 4)).reshape(n_deg, 2, n_deg // 2, n_lat)

    return pack(tab * (w / n_lon)), pack(tab)


def dft_tables(n_lon, n_deg):
    ang = ((np.arange(n_deg)[:, None] * np.arange(n_lon)[None, :]) % n_lon) * (2.0 * math.pi / n_lon)
    c_m = np.where(np.arange(n_deg) == 0, 1.0, 2.0)[:, None, None]
    fwd = np.stack([np.cos(ang), -np.sin(ang)], axis=1)

    def pack(p):
        p = p.astype(np.float32).astype(BF).reshape(2 * n_deg, 2, n_lon // 2)
        return np.ascontiguousarray(np.stack([p, p[:, ::-1]])).reshape(2, 2 * n_deg, n_lon)

    return pack(fwd), pack(c_m * fwd)


def cast_kernel(s_ref, *refs):
    n = len(refs) // 2
    for t in range(n):
        refs[n + t][...] = refs[t][0].astype(BF)


def fwd_dft_kernel(s_ref, tab_ref, *refs):
    pieces, (out, scr, rc) = refs[:8], refs[-3:]
    r = s_ref[2]
    rows = pieces[0].shape[1]
    cols = pieces[0].shape[2]
    nms = out.shape[0]

    def body(c2, carry):
        for u in range(2):
            c = c2 * 2 + u
            for t in range(8):
                row = pl.multiple_of(((t & 3) ^ r) * rows, rows)
                q = t >> 2
                rc[u, pl.ds(row, rows), q * cols:(q + 1) * cols] = pieces[t][c]
        for u in range(2):
            c = c2 * 2 + u
            res = lax.dot_general(tab_ref[0], rc[u], NT, preferred_element_type=F32)
            for j in range(res.shape[1] // 128):
                scr[j, pl.ds(c, nms, stride=16), :] = res[:, j * 128:(j + 1) * 128]
        return carry

    lax.fori_loop(0, 8, body, 0)

    def flush(i, carry):
        for j in range(scr.shape[0]):
            blk = scr[j, pl.ds(pl.multiple_of(i * 512, 512), 512), :]
            out[pl.ds(i * 32, 32), :, j * 128:(j + 1) * 128] = blk.reshape(32, 16, 128).astype(BF)
        return carry

    lax.fori_loop(0, nms // 32, flush, 0)


def fwd_leg_kernel(nf, s_ref, *refs):
    pws, fs = refs[:NV], refs[NV:NV + nf]
    mine, send = refs[-2 * NV:-NV], refs[-NV:]
    h = s_ref[3]
    gran = pl.program_id(0) // (MG // MB)
    nl = pws[0].shape[2]
    for g in range(NV):
        @pl.when(gran == g)
        def _(g=g):
            def body(m8, carry):
                for u in range(8):
                    m = m8 * 8 + u
                    x = jnp.concatenate([f[2 * m + s] for s in range(2) for f in fs], axis=0)
                    p = jnp.concatenate([pws[v][m, h] for v in range(g, NV)] + [pws[v][m, 1 - h] for v in range(g, NV)], axis=0)
                    res = lax.dot_general(p, x, NT, preferred_element_type=F32).astype(BF)
                    for v in range(g, NV):
                        mine[v][m] = res[(v - g) * nl:(v - g + 1) * nl]
                        send[v][m] = res[(NV + v - 2 * g) * nl:(NV + v - 2 * g + 1) * nl]
                return carry

            lax.fori_loop(0, MB // 8, body, 0)


def mix_kernel(vs, s_ref, wre, wim, *refs):
    ins = {v: refs[4 * n:4 * n + 4] for n, v in enumerate(vs)}
    outs = {v: refs[8 + 4 * n:12 + 4 * n] for n, v in enumerate(vs)}
    scr_a, scr_b = refs[-2:]
    h = s_ref[3]
    for n, v in enumerate(vs):
        @pl.when(pl.program_id(0) // 2 == n)
        def _(v=v):
            nm = MG * (v + 1)

            def fill(i, carry):
                rows = pl.ds(pl.multiple_of(i * 512, 512), 512)
                for half in range(2):
                    scr_a[2 * h + half, rows, :] = ins[v][half][pl.ds(i * 32, 32)].astype(F32).reshape(512, 128)
                    scr_a[2 - 2 * h + half, rows, :] = ins[v][2 + half][pl.ds(i * 32, 32)].astype(F32).reshape(512, 128)
                return carry

            lax.fori_loop(0, nm // 32, fill, 0)

            def body(li2, carry):
                for u in range(2):
                    li = li2 * 2 + u
                    lhs = jnp.concatenate([scr_a[b, pl.ds(li, nm, stride=LB), :].astype(BF) for b in range(4)], axis=1)
                    wr, wi = wre[li], wim[li]
                    ni = -wi
                    cg = wr.shape[0] // 4
                    rhs_re = jnp.concatenate([w[b * cg:(b + 1) * cg] for b in range(4) for w in (wr, ni)], axis=0)
                    rhs_im = jnp.concatenate([w[b * cg:(b + 1) * cg] for b in range(4) for w in (wi, wr)], axis=0)
                    bre = jnp.dot(lhs, rhs_re, preferred_element_type=F32)
                    bim = jnp.dot(lhs, rhs_im, preferred_element_type=F32)
                    for b in range(2):
                        scr_b[b, pl.ds(li, nm, stride=LB), :] = bre[:, b * 128:(b + 1) * 128]
                        scr_b[2 + b, pl.ds(li, nm, stride=LB), :] = bim[:, b * 128:(b + 1) * 128]
                return carry

            lax.fori_loop(0, LB // 2, body, 0)
            low = lax.broadcasted_iota(jnp.int32, (512, 128), 1) < 64

            def flush(i, carry):
                rows = pl.ds(pl.multiple_of(i * 512, 512), 512)
                for side, hh in ((0, h), (2, 1 - h)):
                    re, im = scr_b[hh, rows, :], scr_b[2 + hh, rows, :]
                    first = jnp.where(low, re, pltpu.roll(im, 64, 1))
                    second = jnp.where(low, pltpu.roll(re, 64, 1), im)
                    outs[v][side][pl.ds(i * 32, 32)] = first.reshape(32, LB, 128).astype(BF)
                    outs[v][side + 1][pl.ds(i * 32, 32)] = second.reshape(32, LB, 128).astype(BF)
                return carry

            lax.fori_loop(0, nm // 32, flush, 0)


def inv_leg_kernel(s_ref, *refs):
    pis, bm, br = refs[:NV], refs[NV:2 * NV], refs[2 * NV:3 * NV]
    outs = refs[-3:]
    h = s_ref[3]
    gran = pl.program_id(0) // (MG // MB)
    for g in range(NV):
        @pl.when(gran == g)
        def _(g=g):
            def body(m8, carry):
                for u in range(8):
                    m = m8 * 8 + u
                    b = jnp.concatenate([bm[v][m] for v in range(g, NV)] + [br[v][m] for v in range(g, NV)], axis=0)
                    p = jnp.concatenate([pis[v][m, h] for v in range(g, NV)] + [pis[v][m, 1 - h] for v in range(g, NV)], axis=0)
                    y = lax.dot_general(b, p, TN, preferred_element_type=F32).astype(BF)
                    off = 0
                    for o in outs:
                        n = o.shape[1]
                        for s in range(2):
                            o[2 * m + s] = y[s * 64 + off:s * 64 + off + n]
                        off += n
                return carry

            lax.fori_loop(0, MB // 8, body, 0)


def inv_dft_kernel(s_ref, tab_ref, g_ref, *refs):
    pieces, (scr, yc) = refs[-10:-2], refs[-2:]
    r = s_ref[2]
    rows = pieces[0].shape[1]
    cols = pieces[0].shape[2]
    nms = g_ref.shape[0]

    def fill(i, carry):
        for j in range(scr.shape[0]):
            blk = g_ref[pl.ds(i * 32, 32), :, j * 128:(j + 1) * 128].astype(F32)
            scr[j, pl.ds(pl.multiple_of(i * 512, 512), 512), :] = blk.reshape(512, 128)
        return carry

    lax.fori_loop(0, nms // 32, fill, 0)

    def body(c2, carry):
        for u in range(2):
            c = c2 * 2 + u
            g = jnp.concatenate([scr[j, pl.ds(c, nms, stride=16), :].astype(BF) for j in range(scr.shape[0])], axis=1)
            yc[u] = lax.dot_general(g, tab_ref[0], TN, preferred_element_type=F32).astype(BF)
        for u in range(2):
            c = c2 * 2 + u
            for t in range(8):
                row = pl.multiple_of(((t & 3) ^ r) * rows, rows)
                q = t >> 2
                pieces[t][c] = yc[u, pl.ds(row, rows), q * cols:(q + 1) * cols]
        return carry

    lax.fori_loop(0, 8, body, 0)


def call(kernel, grid, in_specs, out_specs, out_shape, flops, nbytes, scratch=(), deps=()):
    fn = pl.pallas_call(
        kernel,
        grid_spec=pltpu.PrefetchScalarGridSpec(
            num_scalar_prefetch=1, grid=grid,
            in_specs=list(in_specs) + [pl.BlockSpec(memory_space=pl.ANY)] * len(deps),
            out_specs=out_specs, scratch_shapes=list(scratch)),
        out_shape=out_shape,
        compiler_params=pltpu.CompilerParams(dimension_semantics=("arbitrary",) * len(grid), vmem_limit_bytes=58 * 2 ** 20),
        cost_estimate=pl.CostEstimate(flops=int(flops), bytes_accessed=int(nbytes), transcendentals=0),
    )
    return lambda *args: fn(*args, *deps)


def solution(mesh):
    lat_devs = mesh.shape['lat']
    lon_devs = mesh.shape['lon']
    nd = lat_devs * lon_devs

    def local_layer(grid_field, mix_weight):
        batch, channels, row_count, col_count = grid_field.shape
        n_lat = row_count * lat_devs
        n_lon = col_count * lon_devs
        n_deg = mix_weight.shape[0]
        half_c = batch * channels // nd
        nms = 2 * n_deg
        lv = n_deg // 2 // NV
        q = lax.axis_index('lon')
        r = lax.axis_index('lat')
        me = q * lat_devs + r
        h = r % 2
        scal = jnp.stack([me, q, r, h]).astype(jnp.int32)
        pw_np, pi_np = legendre_tables(n_lat, n_lon, n_deg)
        tf_np, ti_np = dft_tables(n_lon, n_deg)
        pw, pi, tf, ti = jnp.asarray(pw_np), jnp.asarray(pi_np), jnp.asarray(tf_np), jnp.asarray(ti_np)
        f8 = grid_field.reshape(nd, half_c, row_count, col_count)

        def swap(x, t):
            if t == 0:
                return x
            return lax.ppermute(x, ('lon', 'lat'), [(s, s ^ t) for s in range(nd)])

        def piece(cc):
            return jax.ShapeDtypeStruct((cc, row_count, col_count), BF)

        tab_spec = pl.BlockSpec((1, nms, n_lon), lambda i, s: (s[1], 0, 0))
        piece_spec16 = pl.BlockSpec((16, row_count, col_count), lambda i, s: (i, 0, 0))
        dft_scratch = [pltpu.VMEM((n_lat // 128, nms * 16, 128), F32), pltpu.VMEM((2, n_lat, n_lon), BF)]

        def cast_chunk(c0, cc):
            cb = 8
            base = c0 // cb
            return call(
                cast_kernel, (cc // cb,),
                [pl.BlockSpec((1, cb, row_count, col_count), functools.partial(lambda t, i, s: (s[0] ^ t, base + i, 0, 0), t)) for t in range(nd)],
                [pl.BlockSpec((cb, row_count, col_count), lambda i, s: (i, 0, 0))] * nd,
                [piece(cc)] * nd, 1e6, nd * cc * row_count * col_count * 6)(scal, *([f8] * nd))

        def dft_chunk(pieces, cc, deps):
            return call(
                fwd_dft_kernel, (cc // 16,),
                [tab_spec] + [piece_spec16] * nd,
                pl.BlockSpec((nms, 16, n_lat), lambda i, s: (0, i, 0)),
                jax.ShapeDtypeStruct((nms, cc, n_lat), BF),
                4.0 * cc * nms * n_lat * n_lon, cc * nms * n_lat * 6, dft_scratch, deps)(scal, tf, *pieces)

        last = [MG // MB * (v + 1) - 1 for v in range(NV)]
        tri_specs = [pl.BlockSpec((MB, 2, lv, n_lat), functools.partial(lambda v, i, s: (jnp.minimum(i, last[v]), 0, v, 0), v)) for v in range(NV)]
        spec_specs = [pl.BlockSpec((MB, lv, half_c), functools.partial(lambda v, i, s: (jnp.minimum(i, last[v]), 0, 0), v)) for v in range(NV)]
        spec_shapes = [jax.ShapeDtypeStruct((MG * (v + 1), lv, half_c), BF) for v in range(NV)]

        def f_spec(cc):
            return pl.BlockSpec((2 * MB, cc, n_lat), lambda i, s: (i, 0, 0))

        def leg_fwd(fs):
            res = call(
                functools.partial(fwd_leg_kernel, len(fs)), (n_deg // MB,),
                tri_specs + [f_spec(f.shape[1]) for f in fs],
                spec_specs * 2, spec_shapes * 2,
                1.3 * n_deg * n_deg * n_lat * half_c, 50e6)(scal, *([pw] * NV), *fs)
            return res[:NV], res[NV:]

        def leg_inv(half, mine, recv, deps=()):
            return call(
                inv_leg_kernel, (n_deg // MB,),
                tri_specs + spec_specs * 2,
                [f_spec(cc) for cc in HALVES[half]],
                [jax.ShapeDtypeStruct((nms, cc, n_lat), BF) for cc in HALVES[half]],
                1.3 * n_deg * n_deg * n_lat * half_c, 50e6, (), deps)(scal, *([pi] * NV), *mine, *recv)

        sizes = HALVES[0] + HALVES[1]
        starts = [sum(sizes[:k]) for k in range(len(sizes))]
        recv = []
        for c0, cc in zip(starts, sizes):
            recv.append([swap(p, t) for t, p in enumerate(cast_chunk(c0, cc))])

        w = mix_weight.reshape(n_deg // (2 * LB), 2, LB, channels, channels, 2)
        w = lax.dynamic_index_in_dim(w, h, axis=1, keepdims=False).reshape(n_deg // 2, channels, channels, 2)
        w_re, w_im = w[..., 0], w[..., 1]
        out = jnp.zeros(f8.shape, F32)

        a_mine, a_recv = [], []
        k = 0
        for half in range(2):
            fs = []
            for cc in HALVES[half]:
                deps = []
                if k == 2:
                    deps = [w_re, w_im]
                elif k == 3:
                    deps = [out]
                elif k == len(sizes) - 1:
                    deps = [a_mine[0][0]]
                fs.append(dft_chunk(recv[k], cc, deps))
                k += 1
            mine, send = leg_fwd(fs)
            a_mine.append(mine)
            got = [None] * NV
            for v in reversed(range(NV)):
                got[v] = swap(send[v], 1)
            a_recv.append(got)

        def mix(vs):
            first = vs[0] * 2
            jump = [lambda j: jnp.minimum(j, 1), lambda j: jnp.maximum(j - 2, 0)]
            w_spec = pl.BlockSpec((LB, channels, channels), lambda j, s: (jnp.where(j < 2, first + j, first + j - 4), 0, 0))
            specs, shapes, args = [], [], []
            for n, v in enumerate(vs):
                specs += [pl.BlockSpec((MG * (v + 1), LB, half_c), functools.partial(lambda n, j, s: (0, jump[n](j), 0), n))] * 4
                shapes += [spec_shapes[v]] * 4
                args += [a_mine[0][v], a_mine[1][v], a_recv[0][v], a_recv[1][v]]
            rows = MG * (vs[0] + 1) * LB
            return call(
                functools.partial(mix_kernel, vs), (4,), [w_spec, w_spec] + specs, specs, shapes,
                8.0 * 4 * LB * MG * (vs[0] + 1) * channels * channels, 60e6,
                [pltpu.VMEM((4, rows, 128), F32), pltpu.VMEM((4, rows, 128), F32)])(scal, w_re, w_im, *args)

        b_mine = [[None] * NV, [None] * NV]
        b_recv = [[None] * NV, [None] * NV]
        for vs in ((3, 2), (1, 0)):
            res = mix(vs)
            for n, v in enumerate(vs):
                for half in range(2):
                    b_mine[half][v] = res[4 * n + half]
                    b_recv[half][v] = swap(res[4 * n + 2 + half], 1)

        def idft_chunk(g):
            cc = g.shape[1]
            return call(
                inv_dft_kernel, (cc // 16,),
                [tab_spec, pl.BlockSpec((nms, 16, n_lat), lambda i, s: (0, i, 0))],
                [piece_spec16] * nd, [piece(cc)] * nd,
                4.0 * cc * nms * n_lat * n_lon, cc * nms * n_lat * 6, dft_scratch)(scal, ti, g)

        k = 0
        dep = ()
        for half in range(2):
            for g in leg_inv(half, b_mine[half], b_recv[half], dep):
                cc = g.shape[1]
                pieces = idft_chunk(g)
                if k == 0:
                    dep = (pieces[0],)
                for t, p in enumerate(pieces):
                    y = swap(p, t).astype(F32)
                    src = lax.dynamic_slice(f8, (me ^ t, starts[k], 0, 0), (1, cc, row_count, col_count))
                    new = src + jax.nn.gelu(y, approximate=False)[None]
                    out = lax.dynamic_update_slice(out, new, (me ^ t, starts[k], 0, 0))
                k += 1
        return out.reshape(grid_field.shape)

    field_spec = P('member', None, 'lat', 'lon')
    return jax.shard_map(local_layer, mesh=mesh, in_specs=(field_spec, P()), out_specs=field_spec, check_vma=False)
```

```python
import functools
import math
import numpy as np
import jax
import jax.numpy as jnp
from jax import lax
from jax.experimental import pallas as pl
from jax.experimental.pallas import tpu as pltpu
from jax.sharding import PartitionSpec as P


BF = jnp.bfloat16
F32 = jnp.float32
LB = 16
HALVES = ((16, 48), (32, 16, 16))
MB = 16
MG = 64
NV = 4
NT = (((1,), (1,)), ((), ()))
TN = (((0,), (0,)), ((), ()))


def legendre_tables(n_lat, n_lon, n_deg):
    t = (np.arange(n_lat) + 0.5) * (math.pi / n_lat)
    x = np.cos(t)
    m = np.arange(n_deg)
    steps = np.concatenate([[0.0], np.cumsum(0.5 * np.log((2.0 * m[1:] + 1.0) / (2.0 * m[1:])))])
    diag = np.exp(0.5 * math.log(0.5) + steps[:, None] + m[:, None] * np.log(np.sin(t))[None, :])
    tab = np.zeros((n_deg, n_deg, n_lat))
    mm = m[:, None].astype(np.float64)
    prev1 = np.zeros((n_deg, n_lat))
    prev2 = np.zeros((n_deg, n_lat))
    for l in range(n_deg):
        a = np.sqrt((4.0 * l * l - 1.0) / np.maximum(l * l - mm * mm, 1.0)) if l > 0 else np.ones_like(mm)
        b = np.sqrt(np.maximum((l - 1.0) ** 2 - mm * mm, 0.0) / max(4.0 * (l - 1.0) ** 2 - 1.0, 1.0))
        cur = np.where(mm < l, a * (x[None, :] * prev1 - b * prev2), 0.0)
        cur[l] = diag[l]
        tab[:, l, :] = cur
        prev2 = prev1
        prev1 = cur
    n = np.arange(1, n_lat // 2 + 1)
    series = np.sum(np.cos(2.0 * t[:, None] * n[None, :]) / (4.0 * n * n - 1.0), axis=1)
    w = (2.0 / n_lat) * (1.0 - 2.0 * series)

    def pack(p):
        p = p.astype(np.float32).astype(BF).reshape(n_deg, n_deg // (2 * LB), 2, LB, n_lat)
        return np.ascontiguousarray(p.transpose(0, 2, 1, 3, 4)).reshape(n_deg, 2, n_deg // 2, n_lat)

    return pack(tab * (w / n_lon)), pack(tab)


def dft_tables(n_lon, n_deg):
    ang = ((np.arange(n_deg)[:, None] * np.arange(n_lon)[None, :]) % n_lon) * (2.0 * math.pi / n_lon)
    c_m = np.where(np.arange(n_deg) == 0, 1.0, 2.0)[:, None, None]
    fwd = np.stack([np.cos(ang), -np.sin(ang)], axis=1)

    def pack(p):
        p = p.astype(np.float32).astype(BF).reshape(2 * n_deg, 2, n_lon // 2)
        return np.ascontiguousarray(np.stack([p, p[:, ::-1]])).reshape(2, 2 * n_deg, n_lon)

    return pack(fwd), pack(c_m * fwd)


def cast_kernel(s_ref, *refs):
    n = len(refs) // 2
    for t in range(n):
        refs[n + t][...] = refs[t][0].astype(BF)


def fwd_dft_kernel(s_ref, tab_ref, *refs):
    pieces, (out, scr, rc) = refs[:8], refs[-3:]
    r = s_ref[2]
    rows = pieces[0].shape[1]
    cols = pieces[0].shape[2]
    nms = out.shape[0]

    def body(c2, carry):
        for u in range(2):
            c = c2 * 2 + u
            for t in range(8):
                row = pl.multiple_of(((t & 3) ^ r) * rows, rows)
                q = t >> 2
                rc[u, pl.ds(row, rows), q * cols:(q + 1) * cols] = pieces[t][c]
        for u in range(2):
            c = c2 * 2 + u
            res = lax.dot_general(tab_ref[0], rc[u], NT, preferred_element_type=F32)
            for j in range(res.shape[1] // 128):
                scr[j, pl.ds(c, nms, stride=16), :] = res[:, j * 128:(j + 1) * 128]
        return carry

    lax.fori_loop(0, 8, body, 0)

    def flush(i, carry):
        for j in range(scr.shape[0]):
            blk = scr[j, pl.ds(pl.multiple_of(i * 512, 512), 512), :]
            out[pl.ds(i * 32, 32), :, j * 128:(j + 1) * 128] = blk.reshape(32, 16, 128).astype(BF)
        return carry

    lax.fori_loop(0, nms // 32, flush, 0)


def fwd_leg_kernel(nf, s_ref, *refs):
    pws, fs = refs[:NV], refs[NV:NV + nf]
    mine, send = refs[-2 * NV:-NV], refs[-NV:]
    h = s_ref[3]
    gran = pl.program_id(0) // (MG // MB)
    nl = pws[0].shape[2]
    for g in range(NV):
        @pl.when(gran == g)
        def _(g=g):
            def body(m8, carry):
                for u in range(8):
                    m = m8 * 8 + u
                    x = jnp.concatenate([f[2 * m + s] for s in range(2) for f in fs], axis=0)
                    p = jnp.concatenate([pws[v][m, h] for v in range(g, NV)] + [pws[v][m, 1 - h] for v in range(g, NV)], axis=0)
                    res = lax.dot_general(p, x, NT, preferred_element_type=F32).astype(BF)
                    for v in range(g, NV):
                        mine[v][m] = res[(v - g) * nl:(v - g + 1) * nl]
                        send[v][m] = res[(NV + v - 2 * g) * nl:(NV + v - 2 * g + 1) * nl]
                return carry

            lax.fori_loop(0, MB // 8, body, 0)


def mix_kernel(vs, s_ref, wre, wim, *refs):
    ins = {v: refs[4 * n:4 * n + 4] for n, v in enumerate(vs)}
    outs = {v: refs[8 + 4 * n:12 + 4 * n] for n, v in enumerate(vs)}
    scr_a, scr_b = refs[-2:]
    h = s_ref[3]
    for n, v in enumerate(vs):
        @pl.when(pl.program_id(0) // 2 == n)
        def _(v=v):
            nm = MG * (v + 1)

            def fill(i, carry):
                rows = pl.ds(pl.multiple_of(i * 512, 512), 512)
                for half in range(2):
                    scr_a[2 * h + half, rows, :] = ins[v][half][pl.ds(i * 32, 32)].astype(F32).reshape(512, 128)
                    scr_a[2 - 2 * h + half, rows, :] = ins[v][2 + half][pl.ds(i * 32, 32)].astype(F32).reshape(512, 128)
                return carry

            lax.fori_loop(0, nm // 32, fill, 0)

            def body(li2, carry):
                for u in range(2):
                    li = li2 * 2 + u
                    lhs = jnp.concatenate([scr_a[b, pl.ds(li, nm, stride=LB), :].astype(BF) for b in range(4)], axis=1)
                    wr, wi = wre[li], wim[li]
                    ni = -wi
                    cg = wr.shape[0] // 4
                    rhs_re = jnp.concatenate([w[b * cg:(b + 1) * cg] for b in range(4) for w in (wr, ni)], axis=0)
                    rhs_im = jnp.concatenate([w[b * cg:(b + 1) * cg] for b in range(4) for w in (wi, wr)], axis=0)
                    bre = jnp.dot(lhs, rhs_re, preferred_element_type=F32)
                    bim = jnp.dot(lhs, rhs_im, preferred_element_type=F32)
                    for b in range(2):
                        scr_b[b, pl.ds(li, nm, stride=LB), :] = bre[:, b * 128:(b + 1) * 128]
                        scr_b[2 + b, pl.ds(li, nm, stride=LB), :] = bim[:, b * 128:(b + 1) * 128]
                return carry

            lax.fori_loop(0, LB // 2, body, 0)
            low = lax.broadcasted_iota(jnp.int32, (512, 128), 1) < 64

            def flush(i, carry):
                rows = pl.ds(pl.multiple_of(i * 512, 512), 512)
                for side, hh in ((0, h), (2, 1 - h)):
                    re, im = scr_b[hh, rows, :], scr_b[2 + hh, rows, :]
                    first = jnp.where(low, re, pltpu.roll(im, 64, 1))
                    second = jnp.where(low, pltpu.roll(re, 64, 1), im)
                    outs[v][side][pl.ds(i * 32, 32)] = first.reshape(32, LB, 128).astype(BF)
                    outs[v][side + 1][pl.ds(i * 32, 32)] = second.reshape(32, LB, 128).astype(BF)
                return carry

            lax.fori_loop(0, nm // 32, flush, 0)


def inv_leg_kernel(no, s_ref, *refs):
    pis, bm, br = refs[:NV], refs[NV:2 * NV], refs[2 * NV:3 * NV]
    outs = refs[-no:]
    h = s_ref[3]
    gran = pl.program_id(0) // (MG // MB)
    for g in range(NV):
        @pl.when(gran == g)
        def _(g=g):
            def body(m8, carry):
                for u in range(8):
                    m = m8 * 8 + u
                    b = jnp.concatenate([bm[v][m] for v in range(g, NV)] + [br[v][m] for v in range(g, NV)], axis=0)
                    p = jnp.concatenate([pis[v][m, h] for v in range(g, NV)] + [pis[v][m, 1 - h] for v in range(g, NV)], axis=0)
                    y = lax.dot_general(b, p, TN, preferred_element_type=F32).astype(BF)
                    off = 0
                    for o in outs:
                        n = o.shape[1]
                        for s in range(2):
                            o[2 * m + s] = y[s * 64 + off:s * 64 + off + n]
                        off += n
                return carry

            lax.fori_loop(0, MB // 8, body, 0)


def inv_dft_kernel(s_ref, tab_ref, g_ref, *refs):
    pieces, (scr, yc) = refs[-10:-2], refs[-2:]
    r = s_ref[2]
    rows = pieces[0].shape[1]
    cols = pieces[0].shape[2]
    nms = g_ref.shape[0]

    def fill(i, carry):
        for j in range(scr.shape[0]):
            blk = g_ref[pl.ds(i * 32, 32), :, j * 128:(j + 1) * 128].astype(F32)
            scr[j, pl.ds(pl.multiple_of(i * 512, 512), 512), :] = blk.reshape(512, 128)
        return carry

    lax.fori_loop(0, nms // 32, fill, 0)

    def body(c2, carry):
        for u in range(2):
            c = c2 * 2 + u
            g = jnp.concatenate([scr[j, pl.ds(c, nms, stride=16), :].astype(BF) for j in range(scr.shape[0])], axis=1)
            yc[u] = lax.dot_general(g, tab_ref[0], TN, preferred_element_type=F32).astype(BF)
        for u in range(2):
            c = c2 * 2 + u
            for t in range(8):
                row = pl.multiple_of(((t & 3) ^ r) * rows, rows)
                q = t >> 2
                pieces[t][c] = yc[u, pl.ds(row, rows), q * cols:(q + 1) * cols]
        return carry

    lax.fori_loop(0, 8, body, 0)


def gelu(y):
    return 0.5 * y * (1.0 + lax.erf(y * math.sqrt(0.5)))


def final_kernel(s_ref, f_ref, *refs):
    pieces, (out, buf) = refs[:8], refs[-2:]
    t = pl.program_id(0)
    for n in range(8):
        @pl.when(t == n)
        def _(n=n):
            buf[...] = pieces[n][...]

    def body(c, carry):
        out[0, c] = f_ref[0, c] + gelu(buf[c].astype(F32))
        return carry

    lax.fori_loop(0, buf.shape[0], body, 0)


def call(kernel, grid, in_specs, out_specs, out_shape, flops, nbytes, scratch=(), deps=(), alias=None):
    fn = pl.pallas_call(
        kernel,
        grid_spec=pltpu.PrefetchScalarGridSpec(
            num_scalar_prefetch=1, grid=grid,
            in_specs=list(in_specs) + [pl.BlockSpec(memory_space=pl.ANY)] * len(deps),
            out_specs=out_specs, scratch_shapes=list(scratch)),
        out_shape=out_shape,
        input_output_aliases=alias or {},
        compiler_params=pltpu.CompilerParams(dimension_semantics=("arbitrary",) * len(grid), vmem_limit_bytes=58 * 2 ** 20),
        cost_estimate=pl.CostEstimate(flops=int(flops), bytes_accessed=int(nbytes), transcendentals=0),
    )
    return lambda *args: fn(*args, *deps)


def solution(mesh):
    lat_devs = mesh.shape['lat']
    lon_devs = mesh.shape['lon']
    nd = lat_devs * lon_devs

    def local_layer(grid_field, mix_weight):
        batch, channels, row_count, col_count = grid_field.shape
        n_lat = row_count * lat_devs
        n_lon = col_count * lon_devs
        n_deg = mix_weight.shape[0]
        half_c = batch * channels // nd
        nms = 2 * n_deg
        lv = n_deg // 2 // NV
        q = lax.axis_index('lon')
        r = lax.axis_index('lat')
        me = q * lat_devs + r
        h = r % 2
        scal = jnp.stack([me, q, r, h]).astype(jnp.int32)
        pw_np, pi_np = legendre_tables(n_lat, n_lon, n_deg)
        tf_np, ti_np = dft_tables(n_lon, n_deg)
        pw, pi, tf, ti = jnp.asarray(pw_np), jnp.asarray(pi_np), jnp.asarray(tf_np), jnp.asarray(ti_np)
        f8 = grid_field.reshape(nd, half_c, row_count, col_count)

        def swap(x, t):
            if t == 0:
                return x
            return lax.ppermute(x, ('lon', 'lat'), [(s, s ^ t) for s in range(nd)])

        def piece(cc):
            return jax.ShapeDtypeStruct((cc, row_count, col_count), BF)

        tab_spec = pl.BlockSpec((1, nms, n_lon), lambda i, s: (s[1], 0, 0))
        piece_spec16 = pl.BlockSpec((16, row_count, col_count), lambda i, s: (i, 0, 0))
        dft_scratch = [pltpu.VMEM((n_lat // 128, nms * 16, 128), F32), pltpu.VMEM((2, n_lat, n_lon), BF)]

        def cast_chunk(c0, cc):
            cb = 8
            base = c0 // cb
            return call(
                cast_kernel, (cc // cb,),
                [pl.BlockSpec((1, cb, row_count, col_count), functools.partial(lambda t, i, s: (s[0] ^ t, base + i, 0, 0), t)) for t in range(nd)],
                [pl.BlockSpec((cb, row_count, col_count), lambda i, s: (i, 0, 0))] * nd,
                [piece(cc)] * nd, 1e6, nd * cc * row_count * col_count * 6)(scal, *([f8] * nd))

        def dft_chunk(pieces, cc, deps):
            return call(
                fwd_dft_kernel, (cc // 16,),
                [tab_spec] + [piece_spec16] * nd,
                pl.BlockSpec((nms, 16, n_lat), lambda i, s: (0, i, 0)),
                jax.ShapeDtypeStruct((nms, cc, n_lat), BF),
                4.0 * cc * nms * n_lat * n_lon, cc * nms * n_lat * 6, dft_scratch, deps)(scal, tf, *pieces)

        last = [MG // MB * (v + 1) - 1 for v in range(NV)]
        tri_specs = [pl.BlockSpec((MB, 2, lv, n_lat), functools.partial(lambda v, i, s: (jnp.minimum(i, last[v]), 0, v, 0), v)) for v in range(NV)]
        spec_specs = [pl.BlockSpec((MB, lv, half_c), functools.partial(lambda v, i, s: (jnp.minimum(i, last[v]), 0, 0), v)) for v in range(NV)]
        spec_shapes = [jax.ShapeDtypeStruct((MG * (v + 1), lv, half_c), BF) for v in range(NV)]

        def f_spec(cc):
            return pl.BlockSpec((2 * MB, cc, n_lat), lambda i, s: (i, 0, 0))

        def leg_fwd(fs):
            res = call(
                functools.partial(fwd_leg_kernel, len(fs)), (n_deg // MB,),
                tri_specs + [f_spec(f.shape[1]) for f in fs],
                spec_specs * 2, spec_shapes * 2,
                1.3 * n_deg * n_deg * n_lat * half_c, 50e6)(scal, *([pw] * NV), *fs)
            return res[:NV], res[NV:]

        def leg_inv(half, mine, recv, deps=()):
            return call(
                functools.partial(inv_leg_kernel, len(HALVES[half])), (n_deg // MB,),
                tri_specs + spec_specs * 2,
                [f_spec(cc) for cc in HALVES[half]],
                [jax.ShapeDtypeStruct((nms, cc, n_lat), BF) for cc in HALVES[half]],
                1.3 * n_deg * n_deg * n_lat * half_c, 50e6, (), deps)(scal, *([pi] * NV), *mine, *recv)

        sizes = HALVES[0] + HALVES[1]
        starts = [sum(sizes[:k]) for k in range(len(sizes))]
        recv = []
        for c0, cc in zip(starts, sizes):
            k = len(recv)
            pieces = cast_chunk(c0, cc)
            recv.append([swap(p, t) for t, p in enumerate(pieces)])

        w = mix_weight.reshape(n_deg // (2 * LB), 2, LB, channels, channels, 2)
        w = lax.dynamic_index_in_dim(w, h, axis=1, keepdims=False).reshape(n_deg // 2, channels, channels, 2)
        w_re, w_im = w[..., 0], w[..., 1]

        a_mine, a_recv, prev = [], [], []
        k = 0
        for half in range(2):
            fs = []
            for cc in HALVES[half]:
                deps = list(prev)
                if k == 1:
                    deps += [w_re, w_im]
                elif k == len(HALVES[0]):
                    deps += [a_mine[0][0]]
                fs.append(dft_chunk(recv[k], cc, deps))
                prev = fs[-1:]
                k += 1
            mine, send = leg_fwd(fs)
            a_mine.append(mine)
            got = [None] * NV
            for v in reversed(range(NV)):
                got[v] = swap(send[v], 1)
            a_recv.append(got)

        def mix(vs):
            first = vs[0] * 2
            jump = [lambda j: jnp.minimum(j, 1), lambda j: jnp.maximum(j - 2, 0)]
            w_spec = pl.BlockSpec((LB, channels, channels), lambda j, s: (jnp.where(j < 2, first + j, first + j - 4), 0, 0))
            specs, shapes, args = [], [], []
            for n, v in enumerate(vs):
                specs += [pl.BlockSpec((MG * (v + 1), LB, half_c), functools.partial(lambda n, j, s: (0, jump[n](j), 0), n))] * 4
                shapes += [spec_shapes[v]] * 4
                args += [a_mine[0][v], a_mine[1][v], a_recv[0][v], a_recv[1][v]]
            rows = MG * (vs[0] + 1) * LB
            return call(
                functools.partial(mix_kernel, vs), (4,), [w_spec, w_spec] + specs, specs, shapes,
                8.0 * 4 * LB * MG * (vs[0] + 1) * channels * channels, 60e6,
                [pltpu.VMEM((4, rows, 128), F32), pltpu.VMEM((4, rows, 128), F32)])(scal, w_re, w_im, *args)

        b_mine = [[None] * NV, [None] * NV]
        b_recv = [[None] * NV, [None] * NV]
        for vs in ((3, 2), (1, 0)):
            res = mix(vs)
            for n, v in enumerate(vs):
                for half in range(2):
                    b_mine[half][v] = res[4 * n + half]
                    b_recv[half][v] = swap(res[4 * n + 2 + half], 1)

        def idft_chunk(g):
            cc = g.shape[1]
            return call(
                inv_dft_kernel, (cc // 16,),
                [tab_spec, pl.BlockSpec((nms, 16, n_lat), lambda i, s: (0, i, 0))],
                [piece_spec16] * nd, [piece(cc)] * nd,
                4.0 * cc * nms * n_lat * n_lon, cc * nms * n_lat * 6, dft_scratch)(scal, ti, g)

        def final_chunk(c0, cc, pieces, out):
            cb = 8
            base, nb = c0 // cb, cc // cb
            big = pl.BlockSpec((1, cb, row_count, col_count), lambda t, i, s: (s[0] ^ t, base + i, 0, 0))

            def own(n):
                return pl.BlockSpec((cb, row_count, col_count),
                                    lambda t, i, s: (jnp.where(t == n, i, jnp.where(t < n, 0, nb - 1)), 0, 0))

            deps = [] if out is None else [out]
            return call(
                final_kernel, (nd, nb), [big] + [own(n) for n in range(nd)], big,
                jax.ShapeDtypeStruct(f8.shape, F32), 40 * nd * cc * row_count * col_count, 10 * nd * cc * row_count * col_count,
                [pltpu.VMEM((cb, row_count, col_count), BF)], deps,
                {2 + nd: 0} if deps else None)(scal, f8, *pieces)

        k = 0
        out = None
        dep = ()
        for half in range(2):
            gs = leg_inv(half, b_mine[half], b_recv[half], dep)
            for g in gs:
                cc = g.shape[1]
                pieces = idft_chunk(g)
                if k == 0:
                    dep = (pieces[0],)
                got = [swap(p, t) for t, p in enumerate(pieces)]
                if k < len(sizes) - 1:
                    out = final_chunk(starts[k], cc, got, out)
                else:
                    for t, p in enumerate(got):
                        src = lax.dynamic_slice(f8, (me ^ t, starts[k], 0, 0), (1, cc, row_count, col_count))
                        new = src + gelu(p.astype(F32))[None]
                        out = lax.dynamic_update_slice(out, new, (me ^ t, starts[k], 0, 0))
                k += 1
        return out.reshape(grid_field.shape)

    field_spec = P('member', None, 'lat', 'lon')
    return jax.shard_map(local_layer, mesh=mesh, in_specs=(field_spec, P()), out_specs=field_spec, check_vma=False)
```

```python
import functools
import math
import numpy as np
import jax
import jax.numpy as jnp
from jax import lax
from jax.experimental import pallas as pl
from jax.experimental.pallas import tpu as pltpu
from jax.sharding import PartitionSpec as P


BF = jnp.bfloat16
F32 = jnp.float32
LB = 16
HALVES = ((16, 48), (32, 16, 16))
MB = 32
PAD = LB + 1
MG = 64
NV = 4
NT = (((1,), (1,)), ((), ()))
TN = (((0,), (0,)), ((), ()))


def legendre_tables(n_lat, n_lon, n_deg):
    t = (np.arange(n_lat) + 0.5) * (math.pi / n_lat)
    x = np.cos(t)
    m = np.arange(n_deg)
    steps = np.concatenate([[0.0], np.cumsum(0.5 * np.log((2.0 * m[1:] + 1.0) / (2.0 * m[1:])))])
    diag = np.exp(0.5 * math.log(0.5) + steps[:, None] + m[:, None] * np.log(np.sin(t))[None, :])
    tab = np.zeros((n_deg, n_deg, n_lat))
    mm = m[:, None].astype(np.float64)
    prev1 = np.zeros((n_deg, n_lat))
    prev2 = np.zeros((n_deg, n_lat))
    for l in range(n_deg):
        a = np.sqrt((4.0 * l * l - 1.0) / np.maximum(l * l - mm * mm, 1.0)) if l > 0 else np.ones_like(mm)
        b = np.sqrt(np.maximum((l - 1.0) ** 2 - mm * mm, 0.0) / max(4.0 * (l - 1.0) ** 2 - 1.0, 1.0))
        cur = np.where(mm < l, a * (x[None, :] * prev1 - b * prev2), 0.0)
        cur[l] = diag[l]
        tab[:, l, :] = cur
        prev2 = prev1
        prev1 = cur
    n = np.arange(1, n_lat // 2 + 1)
    series = np.sum(np.cos(2.0 * t[:, None] * n[None, :]) / (4.0 * n * n - 1.0), axis=1)
    w = (2.0 / n_lat) * (1.0 - 2.0 * series)

    def pack(p):
        p = p.astype(np.float32).astype(BF).reshape(n_deg, n_deg // (2 * LB), 2, LB, n_lat)
        return np.ascontiguousarray(p.transpose(0, 2, 1, 3, 4)).reshape(n_deg, 2, n_deg // 2, n_lat)

    return pack(tab * (w / n_lon)), pack(tab)


def dft_tables(n_lon, n_deg):
    ang = ((np.arange(n_deg)[:, None] * np.arange(n_lon)[None, :]) % n_lon) * (2.0 * math.pi / n_lon)
    c_m = np.where(np.arange(n_deg) == 0, 1.0, 2.0)[:, None, None]
    fwd = np.stack([np.cos(ang), -np.sin(ang)], axis=1)

    def pack(p):
        p = p.astype(np.float32).astype(BF).reshape(2 * n_deg, 2, n_lon // 2)
        return np.ascontiguousarray(np.stack([p, p[:, ::-1]])).reshape(2, 2 * n_deg, n_lon)

    return pack(fwd), pack(c_m * fwd)


def cast_kernel(s_ref, *refs):
    n = len(refs) // 2
    for t in range(n):
        refs[n + t][...] = refs[t][0, 0, 0].astype(BF)


def fwd_dft_kernel(s_ref, tab_ref, *refs):
    pieces, (out, scr, rc) = refs[:8], refs[-3:]
    r = s_ref[2]
    rows = pieces[0].shape[1]
    cols = pieces[0].shape[2]
    nms = out.shape[0]

    def body(c2, carry):
        for u in range(2):
            c = c2 * 2 + u
            for t in range(8):
                row = pl.multiple_of(((t & 3) ^ r) * rows, rows)
                q = t >> 2
                rc[u, pl.ds(row, rows), q * cols:(q + 1) * cols] = pieces[t][c]
        for u in range(2):
            c = c2 * 2 + u
            res = lax.dot_general(tab_ref[0], rc[u], NT, preferred_element_type=F32)
            for j in range(res.shape[1] // 128):
                scr[j, pl.ds(c, nms, stride=PAD), :] = res[:, j * 128:(j + 1) * 128]
        return carry

    lax.fori_loop(0, 8, body, 0)

    def flush(i, carry):
        for j in range(scr.shape[0]):
            for u in range(32):
                out[i * 32 + u, :, j * 128:(j + 1) * 128] = scr[j, pl.ds((i * 32 + u) * PAD, LB), :].astype(BF)
        return carry

    lax.fori_loop(0, nms // 32, flush, 0)


def fwd_leg_kernel(nf, s_ref, *refs):
    pws, fs = refs[:NV], refs[NV:NV + nf]
    mine, send = refs[-2 * NV:-NV], refs[-NV:]
    h = s_ref[3]
    gran = pl.program_id(0) // (MG // MB)
    nl = pws[0].shape[2]
    for g in range(NV):
        @pl.when(gran == g)
        def _(g=g):
            def body(m8, carry):
                for u in range(8):
                    m = m8 * 8 + u
                    x = jnp.concatenate([f[2 * m + s] for s in range(2) for f in fs], axis=0)
                    p = jnp.concatenate([pws[v][m, h] for v in range(g, NV)] + [pws[v][m, 1 - h] for v in range(g, NV)], axis=0)
                    res = lax.dot_general(p, x, NT, preferred_element_type=F32).astype(BF)
                    for v in range(g, NV):
                        mine[v][m] = res[(v - g) * nl:(v - g + 1) * nl]
                        send[v][m] = res[(NV + v - 2 * g) * nl:(NV + v - 2 * g + 1) * nl]
                return carry

            lax.fori_loop(0, MB // 8, body, 0)


def mix_kernel(vs, s_ref, wre, wim, *refs):
    ins = {v: refs[4 * n:4 * n + 4] for n, v in enumerate(vs)}
    outs = {v: refs[8 + 2 * n:10 + 2 * n] for n, v in enumerate(vs)}
    scr_a, scr_b = refs[-2:]
    h = s_ref[3]
    for n, v in enumerate(vs):
        @pl.when(pl.program_id(0) // 2 == n)
        def _(v=v):
            nm = MG * (v + 1)

            def fill(i, carry):
                for u in range(16):
                    rows = pl.ds((i * 16 + u) * PAD, LB)
                    for half in range(2):
                        scr_a[2 * half + h, rows, :] = ins[v][half][i * 16 + u].astype(F32)
                        scr_a[2 * half + 1 - h, rows, :] = ins[v][2 + half][i * 16 + u].astype(F32)
                return carry

            lax.fori_loop(0, nm // 16, fill, 0)

            def body(li2, carry):
                for u in range(2):
                    li = li2 * 2 + u
                    lhs = jnp.concatenate([scr_a[b, pl.ds(li, nm, stride=PAD), :].astype(BF) for b in range(4)], axis=1)
                    wr, wi = wre[li], wim[li]
                    ni = -wi
                    cg = wr.shape[0] // 4
                    rhs = jnp.concatenate([jnp.concatenate([w[b * cg:(b + 1) * cg] for b in range(4) for w in pair], axis=0)
                                           for pair in ((wr, ni), (wi, wr))], axis=1)
                    res = jnp.dot(lhs, rhs, preferred_element_type=F32)
                    for b in range(2):
                        scr_b[b, pl.ds(li, nm, stride=PAD), :] = res[:, b * 128:(b + 1) * 128]
                return carry

            lax.fori_loop(0, LB // 2, body, 0)
            low = lax.broadcasted_iota(jnp.int32, (LB, 128), 1) < 64
            first_is_mine = h == 0

            def flush(i, carry):
                for u in range(16):
                    rows = pl.ds((i * 16 + u) * PAD, LB)
                    re, im = scr_b[0, rows, :], scr_b[1, rows, :]
                    zero = jnp.where(low, re, pltpu.roll(im, 64, 1))
                    one = jnp.where(low, pltpu.roll(re, 64, 1), im)
                    outs[v][0][i * 16 + u] = jnp.where(first_is_mine, zero, one).astype(BF)
                    outs[v][1][i * 16 + u] = jnp.where(first_is_mine, one, zero).astype(BF)
                return carry

            lax.fori_loop(0, nm // 16, flush, 0)


def inv_leg_kernel(no, s_ref, *refs):
    pis, bm, br = refs[:NV], refs[NV:2 * NV], refs[2 * NV:3 * NV]
    outs = refs[-no:]
    h = s_ref[3]
    gran = pl.program_id(0) // (MG // MB)
    for g in range(NV):
        @pl.when(gran == g)
        def _(g=g):
            def body(m8, carry):
                for u in range(8):
                    m = m8 * 8 + u
                    b = jnp.concatenate([bm[v][m] for v in range(g, NV)] + [br[v][m] for v in range(g, NV)], axis=0)
                    p = jnp.concatenate([pis[v][m, h] for v in range(g, NV)] + [pis[v][m, 1 - h] for v in range(g, NV)], axis=0)
                    y = lax.dot_general(b, p, TN, preferred_element_type=F32).astype(BF)
                    off = 0
                    for o in outs:
                        n = o.shape[1]
                        for s in range(2):
                            o[2 * m + s] = y[s * 64 + off:s * 64 + off + n]
                        off += n
                return carry

            lax.fori_loop(0, MB // 8, body, 0)


def inv_dft_kernel(s_ref, tab_ref, g_ref, *refs):
    pieces, (scr, yc) = refs[-10:-2], refs[-2:]
    r = s_ref[2]
    rows = pieces[0].shape[1]
    cols = pieces[0].shape[2]
    nms = g_ref.shape[0]

    def fill(i, carry):
        for j in range(scr.shape[0]):
            for u in range(32):
                scr[j, pl.ds((i * 32 + u) * PAD, LB), :] = g_ref[i * 32 + u, :, j * 128:(j + 1) * 128].astype(F32)
        return carry

    lax.fori_loop(0, nms // 32, fill, 0)

    def body(c2, carry):
        for u in range(2):
            c = c2 * 2 + u
            g = jnp.concatenate([scr[j, pl.ds(c, nms, stride=PAD), :].astype(BF) for j in range(scr.shape[0])], axis=1)
            yc[u] = lax.dot_general(g, tab_ref[0], TN, preferred_element_type=F32).astype(BF)
        for u in range(2):
            c = c2 * 2 + u
            for t in range(8):
                row = pl.multiple_of(((t & 3) ^ r) * rows, rows)
                q = t >> 2
                pieces[t][c] = yc[u, pl.ds(row, rows), q * cols:(q + 1) * cols]
        return carry

    lax.fori_loop(0, 8, body, 0)


def gelu(y):
    return 0.5 * y * (1.0 + lax.erf(y * math.sqrt(0.5)))


def final_kernel(s_ref, f_ref, *refs):
    pieces, (out, buf) = refs[:8], refs[-2:]
    t = pl.program_id(0)
    for n in range(8):
        @pl.when(t == n)
        def _(n=n):
            buf[...] = pieces[n][...]

    def body(c, carry):
        out[0, 0, 0, c] = f_ref[0, 0, 0, c] + gelu(buf[c].astype(F32))
        return carry

    lax.fori_loop(0, buf.shape[0], body, 0)


def call(kernel, grid, in_specs, out_specs, out_shape, flops, nbytes, scratch=(), deps=(), alias=None):
    fn = pl.pallas_call(
        kernel,
        grid_spec=pltpu.PrefetchScalarGridSpec(
            num_scalar_prefetch=1, grid=grid,
            in_specs=list(in_specs) + [pl.BlockSpec(memory_space=pl.ANY)] * len(deps),
            out_specs=out_specs, scratch_shapes=list(scratch)),
        out_shape=out_shape,
        input_output_aliases=alias or {},
        compiler_params=pltpu.CompilerParams(dimension_semantics=("arbitrary",) * len(grid), vmem_limit_bytes=58 * 2 ** 20),
        cost_estimate=pl.CostEstimate(flops=int(flops), bytes_accessed=int(nbytes), transcendentals=0),
    )
    return lambda *args: fn(*args, *deps)


def solution(mesh):
    lat_devs = mesh.shape['lat']
    lon_devs = mesh.shape['lon']
    nd = lat_devs * lon_devs

    def local_layer(grid_field, mix_weight):
        batch, channels, row_count, col_count = grid_field.shape
        n_lat = row_count * lat_devs
        n_lon = col_count * lon_devs
        n_deg = mix_weight.shape[0]
        half_c = batch * channels // nd
        nms = 2 * n_deg
        lv = n_deg // 2 // NV
        q = lax.axis_index('lon')
        r = lax.axis_index('lat')
        me = q * lat_devs + r
        h = r % 2
        scal = jnp.stack([me, q, r, h]).astype(jnp.int32)
        pw_np, pi_np = legendre_tables(n_lat, n_lon, n_deg)
        tf_np, ti_np = dft_tables(n_lon, n_deg)
        pw, pi, tf, ti = jnp.asarray(pw_np), jnp.asarray(pi_np), jnp.asarray(tf_np), jnp.asarray(ti_np)
        f6 = grid_field.reshape(batch, 2, channels // half_c, half_c // 2, row_count, col_count)

        def swap(x, t):
            if t == 0:
                return x
            return lax.ppermute(x, ('lon', 'lat'), [(s, s ^ t) for s in range(nd)])

        def piece(cc):
            return jax.ShapeDtypeStruct((cc, row_count, col_count), BF)

        tab_spec = pl.BlockSpec((1, nms, n_lon), lambda i, s: (s[1], 0, 0))
        piece_spec16 = pl.BlockSpec((16, row_count, col_count), lambda i, s: (i, 0, 0))
        dft_scratch = [pltpu.VMEM((n_lat // 128, nms * PAD, 128), F32), pltpu.VMEM((2, n_lat, n_lon), BF)]

        def cast_chunk(half, c0, cc):
            cb = 8
            base = c0 // cb
            return call(
                cast_kernel, (cc // cb,),
                [pl.BlockSpec((1, 1, 1, cb, row_count, col_count),
                              functools.partial(lambda t, i, s: ((s[0] ^ t) // 2, half, (s[0] ^ t) % 2, base + i, 0, 0), t)) for t in range(nd)],
                [pl.BlockSpec((cb, row_count, col_count), lambda i, s: (i, 0, 0))] * nd,
                [piece(cc)] * nd, 1e6, nd * cc * row_count * col_count * 6)(scal, *([f6] * nd))

        def dft_chunk(pieces, cc, deps):
            return call(
                fwd_dft_kernel, (cc // 16,),
                [tab_spec] + [piece_spec16] * nd,
                pl.BlockSpec((nms, 16, n_lat), lambda i, s: (0, i, 0)),
                jax.ShapeDtypeStruct((nms, cc, n_lat), BF),
                4.0 * cc * nms * n_lat * n_lon, cc * nms * n_lat * 6, dft_scratch, deps)(scal, tf, *pieces)

        last = [MG // MB * (v + 1) - 1 for v in range(NV)]
        tri_specs = [pl.BlockSpec((MB, 2, lv, n_lat), functools.partial(lambda v, i, s: (jnp.minimum(i, last[v]), 0, v, 0), v)) for v in range(NV)]
        spec_specs = [pl.BlockSpec((MB, lv, half_c), functools.partial(lambda v, i, s: (jnp.minimum(i, last[v]), 0, 0), v)) for v in range(NV)]
        spec_shapes = [jax.ShapeDtypeStruct((MG * (v + 1), lv, half_c), BF) for v in range(NV)]

        def f_spec(cc):
            return pl.BlockSpec((2 * MB, cc, n_lat), lambda i, s: (i, 0, 0))

        def leg_fwd(fs):
            res = call(
                functools.partial(fwd_leg_kernel, len(fs)), (n_deg // MB,),
                tri_specs + [f_spec(f.shape[1]) for f in fs],
                spec_specs * 2, spec_shapes * 2,
                1.3 * n_deg * n_deg * n_lat * half_c, 50e6)(scal, *([pw] * NV), *fs)
            return res[:NV], res[NV:]

        def leg_inv(half, mine, recv, deps=()):
            return call(
                functools.partial(inv_leg_kernel, len(HALVES[half])), (n_deg // MB,),
                tri_specs + spec_specs * 2,
                [f_spec(cc) for cc in HALVES[half]],
                [jax.ShapeDtypeStruct((nms, cc, n_lat), BF) for cc in HALVES[half]],
                1.3 * n_deg * n_deg * n_lat * half_c, 50e6, (), deps)(scal, *([pi] * NV), *mine, *recv)

        sizes = HALVES[0] + HALVES[1]
        starts = [(half, sum(part[:k])) for half, part in enumerate(HALVES) for k in range(len(part))]
        recv = []
        for (half, c0), cc in zip(starts, sizes):
            k = len(recv)
            pieces = cast_chunk(half, c0, cc)
            recv.append([swap(p, t) for t, p in enumerate(pieces)])

        w = mix_weight.reshape(n_deg // (2 * LB), 2, LB, channels, channels, 2)
        w = lax.dynamic_index_in_dim(w, h, axis=1, keepdims=False).reshape(n_deg // 2, channels, channels, 2)
        w_re, w_im = w[..., 0], w[..., 1]

        a_mine, a_recv, prev = [], [], []
        k = 0
        for half in range(2):
            fs = []
            for cc in HALVES[half]:
                deps = list(prev)
                if k == 1:
                    deps += [w_re, w_im]
                elif k == len(HALVES[0]):
                    deps += [a_mine[0][0]]
                fs.append(dft_chunk(recv[k], cc, deps))
                prev = fs[-1:]
                k += 1
            mine, send = leg_fwd(fs)
            a_mine.append(mine)
            got = [None] * NV
            for v in reversed(range(NV)):
                got[v] = swap(send[v], 1)
            a_recv.append(got)

        def mix(vs, out_half):
            first = vs[0] * 2
            jump = [lambda j: jnp.minimum(j, 1), lambda j: jnp.maximum(j - 2, 0)]
            w_spec = pl.BlockSpec((LB, channels, channels // 2), lambda j, s: (jnp.where(j < 2, first + j, first + j - 4), 0, out_half))
            specs, outs, shapes, args = [], [], [], []
            for n, v in enumerate(vs):
                spec = pl.BlockSpec((MG * (v + 1), LB, half_c), functools.partial(lambda n, j, s: (0, jump[n](j), 0), n))
                specs += [spec] * 4
                outs += [spec] * 2
                shapes += [spec_shapes[v]] * 2
                args += [a_mine[0][v], a_mine[1][v], a_recv[0][v], a_recv[1][v]]
            rows = MG * (vs[0] + 1) * PAD
            return call(
                functools.partial(mix_kernel, vs), (4,), [w_spec, w_spec] + specs, outs, shapes,
                4.0 * 4 * LB * MG * (vs[0] + 1) * channels * channels, 40e6,
                [pltpu.VMEM((4, rows, 128), F32), pltpu.VMEM((2, rows, 128), F32)])(scal, w_re, w_im, *args)

        def mix_half(half):
            mine, recv = [None] * NV, [None] * NV
            for vs in ((3, 2), (1, 0)):
                res = mix(vs, half)
                for n, v in enumerate(vs):
                    mine[v] = res[2 * n]
                    recv[v] = swap(res[2 * n + 1], 1)
            return mine, recv

        def idft_chunk(g):
            cc = g.shape[1]
            return call(
                inv_dft_kernel, (cc // 16,),
                [tab_spec, pl.BlockSpec((nms, 16, n_lat), lambda i, s: (0, i, 0))],
                [piece_spec16] * nd, [piece(cc)] * nd,
                4.0 * cc * nms * n_lat * n_lon, cc * nms * n_lat * 6, dft_scratch)(scal, ti, g)

        def final_chunk(half, c0, cc, pieces, out):
            cb = 8
            base, nb = c0 // cb, cc // cb
            big = pl.BlockSpec((1, 1, 1, cb, row_count, col_count), lambda t, i, s: ((s[0] ^ t) // 2, half, (s[0] ^ t) % 2, base + i, 0, 0))

            def own(n):
                return pl.BlockSpec((cb, row_count, col_count),
                                    lambda t, i, s: (jnp.where(t == n, i, jnp.where(t < n, 0, nb - 1)), 0, 0))

            deps = [] if out is None else [out]
            return call(
                final_kernel, (nd, nb), [big] + [own(n) for n in range(nd)], big,
                jax.ShapeDtypeStruct(f6.shape, F32), 40 * nd * cc * row_count * col_count, 10 * nd * cc * row_count * col_count,
                [pltpu.VMEM((cb, row_count, col_count), BF)], deps,
                {2 + nd: 0} if deps else None)(scal, f6, *pieces)

        k = 0
        out = None
        for half in range(2):
            b_mine, b_recv = mix_half(half)
            gs = leg_inv(half, b_mine, b_recv)
            for g in gs:
                cc = g.shape[1]
                pieces = idft_chunk(g)
                got = [swap(p, t) for t, p in enumerate(pieces)]
                if k < len(sizes) - 1:
                    out = final_chunk(*starts[k], cc, got, out)
                else:
                    for t, p in enumerate(got):
                        at = ((me ^ t) // 2, starts[k][0], (me ^ t) % 2, starts[k][1], 0, 0)
                        src = lax.dynamic_slice(f6, at, (1, 1, 1, cc, row_count, col_count))
                        out = lax.dynamic_update_slice(out, src + gelu(p.astype(F32))[None, None, None], at)
                k += 1
        return out.reshape(grid_field.shape)

    field_spec = P('member', None, 'lat', 'lon')
    return jax.shard_map(local_layer, mesh=mesh, in_specs=(field_spec, P()), out_specs=field_spec, check_vma=False)
```

```python
import functools
import math
import numpy as np
import jax
import jax.numpy as jnp
from jax import lax
from jax.experimental import pallas as pl
from jax.experimental.pallas import tpu as pltpu
from jax.sharding import PartitionSpec as P


BF = jnp.bfloat16
F32 = jnp.float32
LB = 16
HALVES = ((16, 48), (32, 16, 16))
MB = 32
PAD = LB + 1
MG = 64
NV = 4
NT = (((1,), (1,)), ((), ()))
TN = (((0,), (0,)), ((), ()))


def legendre_tables(n_lat, n_lon, n_deg):
    t = (np.arange(n_lat) + 0.5) * (math.pi / n_lat)
    x = np.cos(t)
    m = np.arange(n_deg)
    steps = np.concatenate([[0.0], np.cumsum(0.5 * np.log((2.0 * m[1:] + 1.0) / (2.0 * m[1:])))])
    diag = np.exp(0.5 * math.log(0.5) + steps[:, None] + m[:, None] * np.log(np.sin(t))[None, :])
    tab = np.zeros((n_deg, n_deg, n_lat))
    mm = m[:, None].astype(np.float64)
    prev1 = np.zeros((n_deg, n_lat))
    prev2 = np.zeros((n_deg, n_lat))
    for l in range(n_deg):
        a = np.sqrt((4.0 * l * l - 1.0) / np.maximum(l * l - mm * mm, 1.0)) if l > 0 else np.ones_like(mm)
        b = np.sqrt(np.maximum((l - 1.0) ** 2 - mm * mm, 0.0) / max(4.0 * (l - 1.0) ** 2 - 1.0, 1.0))
        cur = np.where(mm < l, a * (x[None, :] * prev1 - b * prev2), 0.0)
        cur[l] = diag[l]
        tab[:, l, :] = cur
        prev2 = prev1
        prev1 = cur
    n = np.arange(1, n_lat // 2 + 1)
    series = np.sum(np.cos(2.0 * t[:, None] * n[None, :]) / (4.0 * n * n - 1.0), axis=1)
    w = (2.0 / n_lat) * (1.0 - 2.0 * series)

    def pack(p):
        p = p.astype(np.float32).astype(BF).reshape(n_deg, n_deg // (2 * LB), 2, LB, n_lat)
        p = p.transpose(0, 2, 1, 3, 4).reshape(n_deg, 2, NV, n_deg // 2 // NV, n_lat)
        return [np.ascontiguousarray(p[:MG * (v + 1), :, v]) for v in range(NV)]

    return pack(tab * (w / n_lon)), pack(tab)


def dft_tables(n_lon, n_deg):
    ang = ((np.arange(n_deg)[:, None] * np.arange(n_lon)[None, :]) % n_lon) * (2.0 * math.pi / n_lon)
    c_m = np.where(np.arange(n_deg) == 0, 1.0, 2.0)[:, None, None]
    fwd = np.stack([np.cos(ang), -np.sin(ang)], axis=1)

    def pack(p):
        p = p.astype(np.float32).astype(BF).reshape(2 * n_deg, 2, n_lon // 2)
        return np.ascontiguousarray(np.stack([p, p[:, ::-1]])).reshape(2, 2 * n_deg, n_lon)

    return pack(fwd), pack(c_m * fwd)


def cast_kernel(s_ref, *refs):
    n = len(refs) // 2
    for t in range(n):
        refs[n + t][...] = refs[t][0, 0, 0].astype(BF)


def fwd_dft_kernel(s_ref, tab_ref, *refs):
    pieces, (out, scr, rc) = refs[:8], refs[-3:]
    r = s_ref[2]
    rows = pieces[0].shape[1]
    cols = pieces[0].shape[2]
    nms = out.shape[0]

    def body(c2, carry):
        for u in range(2):
            c = c2 * 2 + u
            for t in range(8):
                row = pl.multiple_of(((t & 3) ^ r) * rows, rows)
                q = t >> 2
                rc[u, pl.ds(row, rows), q * cols:(q + 1) * cols] = pieces[t][c]
        for u in range(2):
            c = c2 * 2 + u
            res = lax.dot_general(tab_ref[0], rc[u], NT, preferred_element_type=F32)
            for j in range(res.shape[1] // 128):
                scr[j, pl.ds(c, nms, stride=PAD), :] = res[:, j * 128:(j + 1) * 128]
        return carry

    lax.fori_loop(0, 8, body, 0)

    def flush(i, carry):
        for j in range(scr.shape[0]):
            for u in range(32):
                out[i * 32 + u, :, j * 128:(j + 1) * 128] = scr[j, pl.ds((i * 32 + u) * PAD, LB), :].astype(BF)
        return carry

    lax.fori_loop(0, nms // 32, flush, 0)


def fwd_leg_kernel(nf, s_ref, *refs):
    pws, fs = refs[:NV], refs[NV:NV + nf]
    mine, send = refs[-2 * NV:-NV], refs[-NV:]
    h = s_ref[3]
    gran = pl.program_id(0) // (MG // MB)
    nl = pws[0].shape[2]
    for g in range(NV):
        @pl.when(gran == g)
        def _(g=g):
            def body(m8, carry):
                for u in range(8):
                    m = m8 * 8 + u
                    x = jnp.concatenate([f[2 * m + s] for s in range(2) for f in fs], axis=0)
                    p = jnp.concatenate([pws[v][m, h] for v in range(g, NV)] + [pws[v][m, 1 - h] for v in range(g, NV)], axis=0)
                    res = lax.dot_general(p, x, NT, preferred_element_type=F32).astype(BF)
                    for v in range(g, NV):
                        for b in range(nl // LB):
                            at = (v - g) * nl + b * LB
                            mine[v][b, m] = res[at:at + LB]
                            at += (NV - g) * nl
                            send[v][b, m] = res[at:at + LB]
                return carry

            lax.fori_loop(0, MB // 8, body, 0)


def mix_kernel(vs, s_ref, wre, wim, *refs):
    ins = {v: refs[4 * n:4 * n + 4] for n, v in enumerate(vs)}
    outs = {v: refs[8 + 2 * n:10 + 2 * n] for n, v in enumerate(vs)}
    scr_a, scr_b = refs[-2:]
    h = s_ref[3]
    for n, v in enumerate(vs):
        @pl.when(pl.program_id(0) // 2 == n)
        def _(v=v):
            nm = MG * (v + 1)

            def fill(i, carry):
                for u in range(16):
                    rows = pl.ds((i * 16 + u) * PAD, LB)
                    for half in range(2):
                        scr_a[2 * half + h, rows, :] = ins[v][half][0, i * 16 + u].astype(F32)
                        scr_a[2 * half + 1 - h, rows, :] = ins[v][2 + half][0, i * 16 + u].astype(F32)
                return carry

            lax.fori_loop(0, nm // 16, fill, 0)

            def body(li2, carry):
                for u in range(2):
                    li = li2 * 2 + u
                    lhs = jnp.concatenate([scr_a[b, pl.ds(li, nm, stride=PAD), :].astype(BF) for b in range(4)], axis=1)
                    wr, wi = wre[li], wim[li]
                    ni = -wi
                    cg = wr.shape[0] // 4
                    rhs = jnp.concatenate([jnp.concatenate([w[b * cg:(b + 1) * cg] for b in range(4) for w in pair], axis=0)
                                           for pair in ((wr, ni), (wi, wr))], axis=1)
                    res = jnp.dot(lhs, rhs, preferred_element_type=F32)
                    for b in range(2):
                        scr_b[b, pl.ds(li, nm, stride=PAD), :] = res[:, b * 128:(b + 1) * 128]
                return carry

            lax.fori_loop(0, LB // 2, body, 0)
            low = lax.broadcasted_iota(jnp.int32, (LB, 128), 1) < 64
            first_is_mine = h == 0

            def flush(i, carry):
                for u in range(16):
                    rows = pl.ds((i * 16 + u) * PAD, LB)
                    re, im = scr_b[0, rows, :], scr_b[1, rows, :]
                    zero = jnp.where(low, re, pltpu.roll(im, 64, 1))
                    one = jnp.where(low, pltpu.roll(re, 64, 1), im)
                    outs[v][0][0, i * 16 + u] = jnp.where(first_is_mine, zero, one).astype(BF)
                    outs[v][1][0, i * 16 + u] = jnp.where(first_is_mine, one, zero).astype(BF)
                return carry

            lax.fori_loop(0, nm // 16, flush, 0)


def inv_leg_kernel(no, s_ref, *refs):
    pis, bm, br = refs[:NV], refs[NV:2 * NV], refs[2 * NV:3 * NV]
    outs = refs[-no:]
    h = s_ref[3]
    gran = pl.program_id(0) // (MG // MB)
    for g in range(NV):
        @pl.when(gran == g)
        def _(g=g):
            def body(m8, carry):
                for u in range(8):
                    m = m8 * 8 + u
                    b = jnp.concatenate([x[v][lb, m] for x in (bm, br) for v in range(g, NV) for lb in range(2)], axis=0)
                    p = jnp.concatenate([pis[v][m, h] for v in range(g, NV)] + [pis[v][m, 1 - h] for v in range(g, NV)], axis=0)
                    y = lax.dot_general(b, p, TN, preferred_element_type=F32).astype(BF)
                    off = 0
                    for o in outs:
                        n = o.shape[1]
                        for s in range(2):
                            o[2 * m + s] = y[s * 64 + off:s * 64 + off + n]
                        off += n
                return carry

            lax.fori_loop(0, MB // 8, body, 0)


def inv_dft_kernel(s_ref, tab_ref, g_ref, *refs):
    pieces, (scr, yc) = refs[-10:-2], refs[-2:]
    r = s_ref[2]
    rows = pieces[0].shape[1]
    cols = pieces[0].shape[2]
    nms = g_ref.shape[0]

    def fill(i, carry):
        for j in range(scr.shape[0]):
            for u in range(32):
                scr[j, pl.ds((i * 32 + u) * PAD, LB), :] = g_ref[i * 32 + u, :, j * 128:(j + 1) * 128].astype(F32)
        return carry

    lax.fori_loop(0, nms // 32, fill, 0)

    def body(c2, carry):
        for u in range(2):
            c = c2 * 2 + u
            g = jnp.concatenate([scr[j, pl.ds(c, nms, stride=PAD), :].astype(BF) for j in range(scr.shape[0])], axis=1)
            yc[u] = lax.dot_general(g, tab_ref[0], TN, preferred_element_type=F32).astype(BF)
        for u in range(2):
            c = c2 * 2 + u
            for t in range(8):
                row = pl.multiple_of(((t & 3) ^ r) * rows, rows)
                q = t >> 2
                pieces[t][c] = yc[u, pl.ds(row, rows), q * cols:(q + 1) * cols]
        return carry

    lax.fori_loop(0, 8, body, 0)


def gelu(y):
    return 0.5 * y * (1.0 + lax.erf(y * math.sqrt(0.5)))


def final_kernel(s_ref, f_ref, *refs):
    pieces, (out, buf) = refs[:8], refs[-2:]
    t = pl.program_id(0)
    for n in range(8):
        @pl.when(t == n)
        def _(n=n):
            buf[...] = pieces[n][...]

    def body(c, carry):
        out[0, 0, 0, c] = f_ref[0, 0, 0, c] + gelu(buf[c].astype(F32))
        return carry

    lax.fori_loop(0, buf.shape[0], body, 0)


def call(kernel, grid, in_specs, out_specs, out_shape, flops, nbytes, scratch=(), deps=(), alias=None):
    fn = pl.pallas_call(
        kernel,
        grid_spec=pltpu.PrefetchScalarGridSpec(
            num_scalar_prefetch=1, grid=grid,
            in_specs=list(in_specs) + [pl.BlockSpec(memory_space=pl.ANY)] * len(deps),
            out_specs=out_specs, scratch_shapes=list(scratch)),
        out_shape=out_shape,
        input_output_aliases=alias or {},
        compiler_params=pltpu.CompilerParams(dimension_semantics=("arbitrary",) * len(grid), vmem_limit_bytes=58 * 2 ** 20),
        cost_estimate=pl.CostEstimate(flops=int(flops), bytes_accessed=int(nbytes), transcendentals=0),
    )
    return lambda *args: fn(*args, *deps)


def solution(mesh):
    lat_devs = mesh.shape['lat']
    lon_devs = mesh.shape['lon']
    nd = lat_devs * lon_devs

    def local_layer(grid_field, mix_weight):
        batch, channels, row_count, col_count = grid_field.shape
        n_lat = row_count * lat_devs
        n_lon = col_count * lon_devs
        n_deg = mix_weight.shape[0]
        half_c = batch * channels // nd
        nms = 2 * n_deg
        lv = n_deg // 2 // NV
        q = lax.axis_index('lon')
        r = lax.axis_index('lat')
        me = q * lat_devs + r
        h = r % 2
        scal = jnp.stack([me, q, r, h]).astype(jnp.int32)
        pw_np, pi_np = legendre_tables(n_lat, n_lon, n_deg)
        tf_np, ti_np = dft_tables(n_lon, n_deg)
        pw, pi = [jnp.asarray(x) for x in pw_np], [jnp.asarray(x) for x in pi_np]
        tf, ti = jnp.asarray(tf_np), jnp.asarray(ti_np)
        f6 = grid_field.reshape(batch, 2, channels // half_c, half_c // 2, row_count, col_count)

        def swap(x, t):
            if t == 0:
                return x
            return lax.ppermute(x, ('lon', 'lat'), [(s, s ^ t) for s in range(nd)])

        def piece(cc):
            return jax.ShapeDtypeStruct((cc, row_count, col_count), BF)

        tab_spec = pl.BlockSpec((1, nms, n_lon), lambda i, s: (s[1], 0, 0))
        piece_spec16 = pl.BlockSpec((16, row_count, col_count), lambda i, s: (i, 0, 0))
        dft_scratch = [pltpu.VMEM((n_lat // 128, nms * PAD, 128), F32), pltpu.VMEM((2, n_lat, n_lon), BF)]

        def cast_chunk(half, c0, cc):
            cb = 8
            base = c0 // cb
            return call(
                cast_kernel, (cc // cb,),
                [pl.BlockSpec((1, 1, 1, cb, row_count, col_count),
                              functools.partial(lambda t, i, s: ((s[0] ^ t) // 2, half, (s[0] ^ t) % 2, base + i, 0, 0), t)) for t in range(nd)],
                [pl.BlockSpec((cb, row_count, col_count), lambda i, s: (i, 0, 0))] * nd,
                [piece(cc)] * nd, 1e6, nd * cc * row_count * col_count * 6)(scal, *([f6] * nd))

        def dft_chunk(pieces, cc, deps):
            return call(
                fwd_dft_kernel, (cc // 16,),
                [tab_spec] + [piece_spec16] * nd,
                pl.BlockSpec((nms, 16, n_lat), lambda i, s: (0, i, 0)),
                jax.ShapeDtypeStruct((nms, cc, n_lat), BF),
                4.0 * cc * nms * n_lat * n_lon, cc * nms * n_lat * 6, dft_scratch, deps)(scal, tf, *pieces)

        last = [MG // MB * (v + 1) - 1 for v in range(NV)]
        tri_specs = [pl.BlockSpec((MB, 2, lv, n_lat), functools.partial(lambda v, i, s: (jnp.minimum(i, last[v]), 0, 0, 0), v)) for v in range(NV)]
        spec_specs = [pl.BlockSpec((lv // LB, MB, LB, half_c), functools.partial(lambda v, i, s: (0, jnp.minimum(i, last[v]), 0, 0), v)) for v in range(NV)]
        spec_shapes = [jax.ShapeDtypeStruct((lv // LB, MG * (v + 1), LB, half_c), BF) for v in range(NV)]

        def f_spec(cc):
            return pl.BlockSpec((2 * MB, cc, n_lat), lambda i, s: (i, 0, 0))

        def leg_fwd(fs):
            res = call(
                functools.partial(fwd_leg_kernel, len(fs)), (n_deg // MB,),
                tri_specs + [f_spec(f.shape[1]) for f in fs],
                spec_specs * 2, spec_shapes * 2,
                1.3 * n_deg * n_deg * n_lat * half_c, 50e6)(scal, *pw, *fs)
            return res[:NV], res[NV:]

        def leg_inv(half, mine, recv, deps=()):
            return call(
                functools.partial(inv_leg_kernel, len(HALVES[half])), (n_deg // MB,),
                tri_specs + spec_specs * 2,
                [f_spec(cc) for cc in HALVES[half]],
                [jax.ShapeDtypeStruct((nms, cc, n_lat), BF) for cc in HALVES[half]],
                1.3 * n_deg * n_deg * n_lat * half_c, 50e6, (), deps)(scal, *pi, *mine, *recv)

        sizes = HALVES[0] + HALVES[1]
        starts = [(half, sum(part[:k])) for half, part in enumerate(HALVES) for k in range(len(part))]
        recv = []
        for (half, c0), cc in zip(starts, sizes):
            k = len(recv)
            pieces = cast_chunk(half, c0, cc)
            recv.append([swap(p, t) for t, p in enumerate(pieces)])

        w = mix_weight.reshape(n_deg // (2 * LB), 2, LB, channels, channels, 2)
        w = lax.dynamic_index_in_dim(w, h, axis=1, keepdims=False).reshape(n_deg // 2, channels, channels, 2)
        oh = channels // 2
        w_parts = [[w[:, :, x * oh:(x + 1) * oh, p] for p in range(2)] for x in range(2)]

        a_mine, a_recv, prev = [], [], []
        k = 0
        for half in range(2):
            fs = []
            for cc in HALVES[half]:
                deps = list(prev)
                if k == 1:
                    deps += w_parts[0] + w_parts[1]
                elif k == len(HALVES[0]):
                    deps += [a_mine[0][0]]
                fs.append(dft_chunk(recv[k], cc, deps))
                prev = fs[-1:]
                k += 1
            mine, send = leg_fwd(fs)
            a_mine.append(mine)
            got = [None] * NV
            for v in reversed(range(NV)):
                got[v] = swap(send[v], 1)
            a_recv.append(got)

        def mix(vs, out_half):
            first = vs[0] * 2
            jump = [lambda j: jnp.minimum(j, 1), lambda j: jnp.maximum(j - 2, 0)]
            w_spec = pl.BlockSpec((LB, channels, channels // 2), lambda j, s: (jnp.where(j < 2, first + j, first + j - 4), 0, 0))
            specs, outs, shapes, args = [], [], [], []
            for n, v in enumerate(vs):
                spec = pl.BlockSpec((1, MG * (v + 1), LB, half_c), functools.partial(lambda n, j, s: (jump[n](j), 0, 0, 0), n))
                specs += [spec] * 4
                outs += [spec] * 2
                shapes += [spec_shapes[v]] * 2
                args += [a_mine[0][v], a_mine[1][v], a_recv[0][v], a_recv[1][v]]
            rows = MG * (vs[0] + 1) * PAD
            return call(
                functools.partial(mix_kernel, vs), (4,), [w_spec, w_spec] + specs, outs, shapes,
                4.0 * 4 * LB * MG * (vs[0] + 1) * channels * channels, 40e6,
                [pltpu.VMEM((4, rows, 128), F32), pltpu.VMEM((2, rows, 128), F32)])(scal, *w_parts[out_half], *args)

        def mix_half(half):
            mine, recv = [None] * NV, [None] * NV
            for vs in ((3, 2), (1, 0)):
                res = mix(vs, half)
                for n, v in enumerate(vs):
                    mine[v] = res[2 * n]
                    recv[v] = swap(res[2 * n + 1], 1)
            return mine, recv

        def idft_chunk(g):
            cc = g.shape[1]
            return call(
                inv_dft_kernel, (cc // 16,),
                [tab_spec, pl.BlockSpec((nms, 16, n_lat), lambda i, s: (0, i, 0))],
                [piece_spec16] * nd, [piece(cc)] * nd,
                4.0 * cc * nms * n_lat * n_lon, cc * nms * n_lat * 6, dft_scratch)(scal, ti, g)

        def final_chunk(half, c0, cc, pieces, out):
            cb = 8
            base, nb = c0 // cb, cc // cb
            big = pl.BlockSpec((1, 1, 1, cb, row_count, col_count), lambda t, i, s: ((s[0] ^ t) // 2, half, (s[0] ^ t) % 2, base + i, 0, 0))

            def own(n):
                return pl.BlockSpec((cb, row_count, col_count),
                                    lambda t, i, s: (jnp.where(t == n, i, jnp.where(t < n, 0, nb - 1)), 0, 0))

            deps = [] if out is None else [out]
            return call(
                final_kernel, (nd, nb), [big] + [own(n) for n in range(nd)], big,
                jax.ShapeDtypeStruct(f6.shape, F32), 40 * nd * cc * row_count * col_count, 10 * nd * cc * row_count * col_count,
                [pltpu.VMEM((cb, row_count, col_count), BF)], deps,
                {2 + nd: 0} if deps else None)(scal, f6, *pieces)

        k = 0
        out = None
        for half in range(2):
            b_mine, b_recv = mix_half(half)
            gs = leg_inv(half, b_mine, b_recv)
            for g in gs:
                cc = g.shape[1]
                pieces = idft_chunk(g)
                got = [swap(p, t) for t, p in enumerate(pieces)]
                if k < len(sizes) - 1:
                    out = final_chunk(*starts[k], cc, got, out)
                else:
                    for t, p in enumerate(got):
                        at = ((me ^ t) // 2, starts[k][0], (me ^ t) % 2, starts[k][1], 0, 0)
                        src = lax.dynamic_slice(f6, at, (1, 1, 1, cc, row_count, col_count))
                        out = lax.dynamic_update_slice(out, src + gelu(p.astype(F32))[None, None, None], at)
                k += 1
        return out.reshape(grid_field.shape)

    field_spec = P('member', None, 'lat', 'lon')
    return jax.shard_map(local_layer, mesh=mesh, in_specs=(field_spec, P()), out_specs=field_spec, check_vma=False)
```

```python
import functools
import math
import numpy as np
import jax
import jax.numpy as jnp
from jax import lax
from jax.experimental import pallas as pl
from jax.experimental.pallas import tpu as pltpu
from jax.sharding import PartitionSpec as P


BF = jnp.bfloat16
F32 = jnp.float32
LB = 16
HALVES = ((16, 48), (32, 16, 16))
MB = 32
PAD = LB + 1
MG = 64
NV = 4
MIX = ((1, 0), (3,), (2,))
NT = (((1,), (1,)), ((), ()))
TN = (((0,), (0,)), ((), ()))


def legendre_tables(n_lat, n_lon, n_deg):
    t = (np.arange(n_lat) + 0.5) * (math.pi / n_lat)
    x = np.cos(t)
    m = np.arange(n_deg)
    steps = np.concatenate([[0.0], np.cumsum(0.5 * np.log((2.0 * m[1:] + 1.0) / (2.0 * m[1:])))])
    diag = np.exp(0.5 * math.log(0.5) + steps[:, None] + m[:, None] * np.log(np.sin(t))[None, :])
    tab = np.zeros((n_deg, n_deg, n_lat))
    mm = m[:, None].astype(np.float64)
    prev1 = np.zeros((n_deg, n_lat))
    prev2 = np.zeros((n_deg, n_lat))
    for l in range(n_deg):
        a = np.sqrt((4.0 * l * l - 1.0) / np.maximum(l * l - mm * mm, 1.0)) if l > 0 else np.ones_like(mm)
        b = np.sqrt(np.maximum((l - 1.0) ** 2 - mm * mm, 0.0) / max(4.0 * (l - 1.0) ** 2 - 1.0, 1.0))
        cur = np.where(mm < l, a * (x[None, :] * prev1 - b * prev2), 0.0)
        cur[l] = diag[l]
        tab[:, l, :] = cur
        prev2 = prev1
        prev1 = cur
    n = np.arange(1, n_lat // 2 + 1)
    series = np.sum(np.cos(2.0 * t[:, None] * n[None, :]) / (4.0 * n * n - 1.0), axis=1)
    w = (2.0 / n_lat) * (1.0 - 2.0 * series)

    def pack(p):
        p = p.astype(np.float32).astype(BF).reshape(n_deg, n_deg // (2 * LB), 2, LB, n_lat)
        p = p.transpose(0, 2, 1, 3, 4).reshape(n_deg, 2, NV, n_deg // 2 // NV, n_lat)
        return [np.ascontiguousarray(p[:MG * (v + 1), :, v]) for v in range(NV)]

    return pack(tab * (w / n_lon)), pack(tab)


def dft_tables(n_lon, n_deg):
    ang = ((np.arange(n_deg)[:, None] * np.arange(n_lon)[None, :]) % n_lon) * (2.0 * math.pi / n_lon)
    c_m = np.where(np.arange(n_deg) == 0, 1.0, 2.0)[:, None, None]
    fwd = np.stack([np.cos(ang), -np.sin(ang)], axis=1)

    def pack(p):
        p = p.astype(np.float32).astype(BF).reshape(2 * n_deg, 2, n_lon // 2)
        return np.ascontiguousarray(np.stack([p, p[:, ::-1]])).reshape(2, 2 * n_deg, n_lon)

    return pack(fwd), pack(c_m * fwd)


def cast_kernel(s_ref, *refs):
    n = len(refs) // 2
    for t in range(n):
        refs[n + t][...] = refs[t][0, 0, 0].astype(BF)


def fwd_dft_kernel(s_ref, tab_ref, *refs):
    pieces, (out, scr, rc) = refs[:8], refs[-3:]
    r = s_ref[2]
    rows = pieces[0].shape[1]
    cols = pieces[0].shape[2]
    nms, nb = out.shape[0], out.shape[1]

    def body(c2, carry):
        for u in range(2):
            c = c2 * 2 + u
            for t in range(8):
                row = pl.multiple_of(((t & 3) ^ r) * rows, rows)
                q = t >> 2
                rc[u, pl.ds(row, rows), q * cols:(q + 1) * cols] = pieces[t][c]
        for u in range(2):
            c = c2 * 2 + u
            res = lax.dot_general(tab_ref[0], rc[u], NT, preferred_element_type=F32)
            for j in range(res.shape[1] // 128):
                scr[j, pl.ds(c, nms, stride=nb + 1), :] = res[:, j * 128:(j + 1) * 128]
        return carry

    lax.fori_loop(0, nb // 2, body, 0)

    def flush(i, carry):
        for j in range(scr.shape[0]):
            for u in range(32):
                out[i * 32 + u, :, j * 128:(j + 1) * 128] = scr[j, pl.ds((i * 32 + u) * (nb + 1), nb), :].astype(BF)
        return carry

    lax.fori_loop(0, nms // 32, flush, 0)


def fwd_leg_kernel(nf, s_ref, *refs):
    pws, fs = refs[:NV], refs[NV:NV + nf]
    mine, send = refs[-2 * NV:-NV], refs[-NV:]
    h = s_ref[3]
    gran = pl.program_id(0) // (MG // MB)
    nl = pws[0].shape[2]
    for g in range(NV):
        @pl.when(gran == g)
        def _(g=g):
            def body(m8, carry):
                for u in range(8):
                    m = m8 * 8 + u
                    x = jnp.concatenate([f[2 * m + s] for s in range(2) for f in fs], axis=0)
                    p = jnp.concatenate([pws[v][m, h] for v in range(g, NV)] + [pws[v][m, 1 - h] for v in range(g, NV)], axis=0)
                    res = lax.dot_general(p, x, NT, preferred_element_type=F32).astype(BF)
                    for v in range(g, NV):
                        for b in range(nl // LB):
                            at = (v - g) * nl + b * LB
                            mine[v][b, m] = res[at:at + LB]
                            at += (NV - g) * nl
                            send[v][b, m] = res[at:at + LB]
                return carry

            lax.fori_loop(0, MB // 8, body, 0)


def mix_kernel(vs, s_ref, wre, wim, *refs):
    ins = {v: refs[4 * n:4 * n + 4] for n, v in enumerate(vs)}
    outs = {v: refs[4 * len(vs) + 2 * n:4 * len(vs) + 2 * n + 2] for n, v in enumerate(vs)}
    scr_a, scr_b = refs[-2:]
    h = s_ref[3]
    for n, v in enumerate(vs):
        @pl.when(pl.program_id(0) // 2 == n)
        def _(v=v):
            nm = MG * (v + 1)

            def fill(i, carry):
                for u in range(16):
                    rows = pl.ds((i * 16 + u) * PAD, LB)
                    for half in range(2):
                        scr_a[2 * half + h, rows, :] = ins[v][half][0, i * 16 + u].astype(F32)
                        scr_a[2 * half + 1 - h, rows, :] = ins[v][2 + half][0, i * 16 + u].astype(F32)
                return carry

            lax.fori_loop(0, nm // 16, fill, 0)

            def body(li2, carry):
                for u in range(2):
                    li = li2 * 2 + u
                    lhs = jnp.concatenate([scr_a[b, pl.ds(li, nm, stride=PAD), :].astype(BF) for b in range(4)], axis=1)
                    wr, wi = wre[li], wim[li]
                    ni = -wi
                    cg = wr.shape[0] // 4
                    rhs = jnp.concatenate([jnp.concatenate([w[b * cg:(b + 1) * cg] for b in range(4) for w in pair], axis=0)
                                           for pair in ((wr, ni), (wi, wr))], axis=1)
                    res = jnp.dot(lhs, rhs, preferred_element_type=F32)
                    for b in range(2):
                        scr_b[b, pl.ds(li, nm, stride=PAD), :] = res[:, b * 128:(b + 1) * 128]
                return carry

            lax.fori_loop(0, LB // 2, body, 0)
            low = lax.broadcasted_iota(jnp.int32, (LB, 128), 1) < 64
            first_is_mine = h == 0

            def flush(i, carry):
                for u in range(16):
                    rows = pl.ds((i * 16 + u) * PAD, LB)
                    re, im = scr_b[0, rows, :], scr_b[1, rows, :]
                    zero = jnp.where(low, re, pltpu.roll(im, 64, 1))
                    one = jnp.where(low, pltpu.roll(re, 64, 1), im)
                    outs[v][0][0, i * 16 + u] = jnp.where(first_is_mine, zero, one).astype(BF)
                    outs[v][1][0, i * 16 + u] = jnp.where(first_is_mine, one, zero).astype(BF)
                return carry

            lax.fori_loop(0, nm // 16, flush, 0)


def inv_leg_kernel(offs, s_ref, *refs):
    pis, bm, br = refs[:NV], refs[NV:2 * NV], refs[2 * NV:3 * NV]
    outs = refs[-len(offs):]
    h = s_ref[3]
    gran = pl.program_id(0) // (MG // MB)
    for g in range(NV):
        @pl.when(gran == g)
        def _(g=g):
            def body(m8, carry):
                for u in range(8):
                    m = m8 * 8 + u
                    b = jnp.concatenate([x[v][lb, m] for x in (bm, br) for v in range(g, NV) for lb in range(2)], axis=0)
                    p = jnp.concatenate([pis[v][m, h] for v in range(g, NV)] + [pis[v][m, 1 - h] for v in range(g, NV)], axis=0)
                    y = lax.dot_general(b, p, TN, preferred_element_type=F32).astype(BF)
                    for o, off in zip(outs, offs):
                        n = o.shape[1]
                        for s in range(2):
                            o[2 * m + s] = y[s * 64 + off:s * 64 + off + n]
                return carry

            lax.fori_loop(0, MB // 8, body, 0)


def inv_dft_kernel(s_ref, tab_ref, g_ref, *refs):
    pieces, (scr, yc) = refs[-10:-2], refs[-2:]
    r = s_ref[2]
    rows = pieces[0].shape[1]
    cols = pieces[0].shape[2]
    nms, nb = g_ref.shape[0], g_ref.shape[1]

    def fill(i, carry):
        for j in range(scr.shape[0]):
            for u in range(32):
                scr[j, pl.ds((i * 32 + u) * (nb + 1), nb), :] = g_ref[i * 32 + u, :, j * 128:(j + 1) * 128].astype(F32)
        return carry

    lax.fori_loop(0, nms // 32, fill, 0)

    def body(c2, carry):
        for u in range(2):
            c = c2 * 2 + u
            g = jnp.concatenate([scr[j, pl.ds(c, nms, stride=nb + 1), :].astype(BF) for j in range(scr.shape[0])], axis=1)
            yc[u] = lax.dot_general(g, tab_ref[0], TN, preferred_element_type=F32).astype(BF)
        for u in range(2):
            c = c2 * 2 + u
            for t in range(8):
                row = pl.multiple_of(((t & 3) ^ r) * rows, rows)
                q = t >> 2
                pieces[t][c] = yc[u, pl.ds(row, rows), q * cols:(q + 1) * cols]
        return carry

    lax.fori_loop(0, nb // 2, body, 0)


def gelu(y):
    return 0.5 * y * (1.0 + lax.erf(y * math.sqrt(0.5)))


def final_kernel(s_ref, f_ref, *refs):
    pieces, (out, buf) = refs[:8], refs[-2:]
    t = pl.program_id(0)
    for n in range(8):
        @pl.when(t == n)
        def _(n=n):
            buf[...] = pieces[n][...]

    def body(c, carry):
        out[0, 0, 0, c] = f_ref[0, 0, 0, c] + gelu(buf[c].astype(F32))
        return carry

    lax.fori_loop(0, buf.shape[0], body, 0)


def call(kernel, grid, in_specs, out_specs, out_shape, flops, nbytes, scratch=(), deps=(), alias=None, vmem=32):
    fn = pl.pallas_call(
        kernel,
        grid_spec=pltpu.PrefetchScalarGridSpec(
            num_scalar_prefetch=1, grid=grid,
            in_specs=list(in_specs) + [pl.BlockSpec(memory_space=pl.ANY)] * len(deps),
            out_specs=out_specs, scratch_shapes=list(scratch)),
        out_shape=out_shape,
        input_output_aliases=alias or {},
        compiler_params=pltpu.CompilerParams(dimension_semantics=("arbitrary",) * len(grid), vmem_limit_bytes=vmem * 2 ** 20),
        cost_estimate=pl.CostEstimate(flops=int(flops), bytes_accessed=int(nbytes), transcendentals=0),
    )
    return lambda *args: fn(*args, *deps)


def solution(mesh):
    lat_devs = mesh.shape['lat']
    lon_devs = mesh.shape['lon']
    nd = lat_devs * lon_devs

    def local_layer(grid_field, mix_weight):
        batch, channels, row_count, col_count = grid_field.shape
        n_lat = row_count * lat_devs
        n_lon = col_count * lon_devs
        n_deg = mix_weight.shape[0]
        half_c = batch * channels // nd
        nms = 2 * n_deg
        lv = n_deg // 2 // NV
        q = lax.axis_index('lon')
        r = lax.axis_index('lat')
        me = q * lat_devs + r
        h = r % 2
        scal = jnp.stack([me, q, r, h]).astype(jnp.int32)
        pw_np, pi_np = legendre_tables(n_lat, n_lon, n_deg)
        tf_np, ti_np = dft_tables(n_lon, n_deg)
        pw, pi = [jnp.asarray(x) for x in pw_np], [jnp.asarray(x) for x in pi_np]
        tf, ti = jnp.asarray(tf_np), jnp.asarray(ti_np)
        f6 = grid_field.reshape(batch, 2, channels // half_c, half_c // 2, row_count, col_count)

        def swap(x, t):
            if t == 0:
                return x
            return lax.ppermute(x, ('lon', 'lat'), [(s, s ^ t) for s in range(nd)])

        def piece(cc):
            return jax.ShapeDtypeStruct((cc, row_count, col_count), BF)

        tab_spec = pl.BlockSpec((1, nms, n_lon), lambda i, s: (s[1], 0, 0))

        def piece_spec(nb):
            return pl.BlockSpec((nb, row_count, col_count), lambda i, s: (i, 0, 0))

        def dft_scratch(nb):
            return [pltpu.VMEM((n_lat // 128, nms * (nb + 1), 128), F32), pltpu.VMEM((2, n_lat, n_lon), BF)]

        def cast_chunk(half, c0, cc):
            cb = 8
            base = c0 // cb
            return call(
                cast_kernel, (cc // cb,),
                [pl.BlockSpec((1, 1, 1, cb, row_count, col_count),
                              functools.partial(lambda t, i, s: ((s[0] ^ t) // 2, half, (s[0] ^ t) % 2, base + i, 0, 0), t)) for t in range(nd)],
                [pl.BlockSpec((cb, row_count, col_count), lambda i, s: (i, 0, 0))] * nd,
                [piece(cc)] * nd, 1e6, nd * cc * row_count * col_count * 6, vmem=16)(scal, *([f6] * nd))

        def dft_chunk(pieces, cc, nb, deps):
            return call(
                fwd_dft_kernel, (cc // nb,),
                [tab_spec] + [piece_spec(nb)] * nd,
                pl.BlockSpec((nms, nb, n_lat), lambda i, s: (0, i, 0)),
                jax.ShapeDtypeStruct((nms, cc, n_lat), BF),
                4.0 * cc * nms * n_lat * n_lon, cc * nms * n_lat * 6, dft_scratch(nb), deps)(scal, tf, *pieces)

        last = [MG // MB * (v + 1) - 1 for v in range(NV)]
        tri_specs = [pl.BlockSpec((MB, 2, lv, n_lat), functools.partial(lambda v, i, s: (jnp.minimum(i, last[v]), 0, 0, 0), v)) for v in range(NV)]
        spec_specs = [pl.BlockSpec((lv // LB, MB, LB, half_c), functools.partial(lambda v, i, s: (0, jnp.minimum(i, last[v]), 0, 0), v)) for v in range(NV)]
        spec_shapes = [jax.ShapeDtypeStruct((lv // LB, MG * (v + 1), LB, half_c), BF) for v in range(NV)]

        def f_spec(cc):
            return pl.BlockSpec((2 * MB, cc, n_lat), lambda i, s: (i, 0, 0))

        def leg_fwd(fs):
            res = call(
                functools.partial(fwd_leg_kernel, len(fs)), (n_deg // MB,),
                tri_specs + [f_spec(f.shape[1]) for f in fs],
                spec_specs * 2, spec_shapes * 2,
                1.3 * n_deg * n_deg * n_lat * half_c, 50e6, vmem=26)(scal, *pw, *fs)
            return res[:NV], res[NV:]

        def leg_inv(offs, ccs, mine, recv):
            return call(
                functools.partial(inv_leg_kernel, offs), (n_deg // MB,),
                tri_specs + spec_specs * 2,
                [f_spec(cc) for cc in ccs],
                [jax.ShapeDtypeStruct((nms, cc, n_lat), BF) for cc in ccs],
                1.3 * n_deg * n_deg * n_lat * half_c, 50e6, vmem=26)(scal, *pi, *mine, *recv)

        sizes = HALVES[0] + HALVES[1]
        starts = [(half, sum(part[:k])) for half, part in enumerate(HALVES) for k in range(len(part))]
        recv = []
        for (half, c0), cc in zip(starts, sizes):
            k = len(recv)
            pieces = cast_chunk(half, c0, cc)
            recv.append([swap(p, t) for t, p in enumerate(pieces)])

        w = mix_weight.reshape(n_deg // (2 * LB), 2, LB, channels, channels, 2)
        w = lax.dynamic_index_in_dim(w, h, axis=1, keepdims=False).reshape(n_deg // 2, channels, channels, 2)
        oh = channels // 2
        w_parts = [[w[:, :, x * oh:(x + 1) * oh, p] for p in range(2)] for x in range(2)]

        a_mine, a_recv, prev = [], [], []
        k = 0
        for half in range(2):
            fs = []
            for cc in HALVES[half]:
                deps = list(prev)
                if k == 1:
                    deps += w_parts[0] + w_parts[1]
                elif k == len(HALVES[0]):
                    deps += [a_mine[0][0]]
                fs.append(dft_chunk(recv[k], cc, 8 if k == len(sizes) - 1 else 16, deps))
                prev = fs[-1:]
                k += 1
            mine, send = leg_fwd(fs)
            a_mine.append(mine)
            got = [None] * NV
            for v in sum(MIX, ()):
                got[v] = swap(send[v], 1)
            a_recv.append(got)

        def mix(vs, out_half):
            jump = [lambda j: jnp.minimum(j, 1), lambda j: jnp.maximum(j - 2, 0)]
            w_spec = pl.BlockSpec((LB, channels, channels // 2), lambda j, s: (jnp.where(j < 2, 2 * vs[0] + j, 2 * vs[-1] + j - 2), 0, 0))
            specs, outs, shapes, args = [], [], [], []
            for n, v in enumerate(vs):
                spec = pl.BlockSpec((1, MG * (v + 1), LB, half_c), functools.partial(lambda n, j, s: (jump[n](j), 0, 0, 0), n))
                specs += [spec] * 4
                outs += [spec] * 2
                shapes += [spec_shapes[v]] * 2
                args += [a_mine[0][v], a_mine[1][v], a_recv[0][v], a_recv[1][v]]
            rows = MG * (vs[0] + 1) * PAD
            return call(
                functools.partial(mix_kernel, vs), (2 * len(vs),), [w_spec, w_spec] + specs, outs, shapes,
                4.0 * 4 * LB * MG * (vs[0] + 1) * channels * channels, 40e6,
                [pltpu.VMEM((4, rows, 128), F32), pltpu.VMEM((2, rows, 128), F32)], vmem=40)(scal, *w_parts[out_half], *args)

        def mix_half(half):
            mine, recv = [None] * NV, [None] * NV
            for vs in MIX:
                res = mix(vs, half)
                for n, v in enumerate(vs):
                    mine[v] = res[2 * n]
                    recv[v] = swap(res[2 * n + 1], 1)
            return mine, recv

        def idft_chunk(g, nb):
            cc = g.shape[1]
            return call(
                inv_dft_kernel, (cc // nb,),
                [tab_spec, pl.BlockSpec((nms, nb, n_lat), lambda i, s: (0, i, 0))],
                [piece_spec(nb)] * nd, [piece(cc)] * nd,
                4.0 * cc * nms * n_lat * n_lon, cc * nms * n_lat * 6, dft_scratch(nb))(scal, ti, g)

        def final_chunk(half, c0, cc, pieces, out):
            cb = 8
            base, nb = c0 // cb, cc // cb
            big = pl.BlockSpec((1, 1, 1, cb, row_count, col_count), lambda t, i, s: ((s[0] ^ t) // 2, half, (s[0] ^ t) % 2, base + i, 0, 0))

            def own(n):
                return pl.BlockSpec((cb, row_count, col_count),
                                    lambda t, i, s: (jnp.where(t == n, i, jnp.where(t < n, 0, nb - 1)), 0, 0))

            deps = [] if out is None else [out]
            return call(
                final_kernel, (nd, nb), [big] + [own(n) for n in range(nd)], big,
                jax.ShapeDtypeStruct(f6.shape, F32), 40 * nd * cc * row_count * col_count, 10 * nd * cc * row_count * col_count,
                [pltpu.VMEM((cb, row_count, col_count), BF)], deps,
                {2 + nd: 0} if deps else None, 16)(scal, f6, *pieces)

        k = 0
        out = None
        for half in range(2):
            b_mine, b_recv = mix_half(half)
            offs = [c0 for hf, c0 in starts if hf == half]
            groups = [[0], list(range(1, len(offs)))] if half == 0 else [list(range(len(offs)))]
            gs = []
            for group in groups:
                gs += leg_inv([offs[x] for x in group], [HALVES[half][x] for x in group], b_mine, b_recv)
            for g in gs:
                cc = g.shape[1]
                pieces = idft_chunk(g, 8 if k == 0 else 16)
                got = [swap(p, t) for t, p in enumerate(pieces)]
                if k < len(sizes) - 1:
                    out = final_chunk(*starts[k], cc, got, out)
                else:
                    for t, p in enumerate(got):
                        at = ((me ^ t) // 2, starts[k][0], (me ^ t) % 2, starts[k][1], 0, 0)
                        src = lax.dynamic_slice(f6, at, (1, 1, 1, cc, row_count, col_count))
                        out = lax.dynamic_update_slice(out, src + gelu(p.astype(F32))[None, None, None], at)
                k += 1
        return out.reshape(grid_field.shape)

    field_spec = P('member', None, 'lat', 'lon')
    return jax.shard_map(local_layer, mesh=mesh, in_specs=(field_spec, P()), out_specs=field_spec, check_vma=False)
```

```python
import functools
import math
import numpy as np
import jax
import jax.numpy as jnp
from jax import lax
from jax.experimental import pallas as pl
from jax.experimental.pallas import tpu as pltpu
from jax.sharding import PartitionSpec as P


BF = jnp.bfloat16
F32 = jnp.float32
LB = 16
HALVES = ((16, 48), (32, 16, 16))
MB = 32
PAD = LB + 1
MG = 64
NV = 4
MIX = ((1, 0), (3, 2))
NT = (((1,), (1,)), ((), ()))
TN = (((0,), (0,)), ((), ()))


def legendre_tables(n_lat, n_lon, n_deg):
    t = (np.arange(n_lat) + 0.5) * (math.pi / n_lat)
    x = np.cos(t)
    m = np.arange(n_deg)
    steps = np.concatenate([[0.0], np.cumsum(0.5 * np.log((2.0 * m[1:] + 1.0) / (2.0 * m[1:])))])
    diag = np.exp(0.5 * math.log(0.5) + steps[:, None] + m[:, None] * np.log(np.sin(t))[None, :])
    tab = np.zeros((n_deg, n_deg, n_lat))
    mm = m[:, None].astype(np.float64)
    prev1 = np.zeros((n_deg, n_lat))
    prev2 = np.zeros((n_deg, n_lat))
    for l in range(n_deg):
        a = np.sqrt((4.0 * l * l - 1.0) / np.maximum(l * l - mm * mm, 1.0)) if l > 0 else np.ones_like(mm)
        b = np.sqrt(np.maximum((l - 1.0) ** 2 - mm * mm, 0.0) / max(4.0 * (l - 1.0) ** 2 - 1.0, 1.0))
        cur = np.where(mm < l, a * (x[None, :] * prev1 - b * prev2), 0.0)
        cur[l] = diag[l]
        tab[:, l, :] = cur
        prev2 = prev1
        prev1 = cur
    n = np.arange(1, n_lat // 2 + 1)
    series = np.sum(np.cos(2.0 * t[:, None] * n[None, :]) / (4.0 * n * n - 1.0), axis=1)
    w = (2.0 / n_lat) * (1.0 - 2.0 * series)

    def pack(p):
        p = p.astype(np.float32).astype(BF).reshape(n_deg, n_deg // (2 * LB), 2, LB, n_lat)
        p = p.transpose(0, 2, 1, 3, 4).reshape(n_deg, 2, NV, n_deg // 2 // NV, n_lat)
        return [np.ascontiguousarray(p[:MG * (v + 1), :, v]) for v in range(NV)]

    return pack(tab * (w / n_lon)), pack(tab)


def dft_tables(n_lon, n_deg):
    ang = ((np.arange(n_deg)[:, None] * np.arange(n_lon)[None, :]) % n_lon) * (2.0 * math.pi / n_lon)
    c_m = np.where(np.arange(n_deg) == 0, 1.0, 2.0)[:, None, None]
    fwd = np.stack([np.cos(ang), -np.sin(ang)], axis=1)

    def pack(p):
        p = p.astype(np.float32).astype(BF).reshape(2 * n_deg, 2, n_lon // 2)
        return np.ascontiguousarray(np.stack([p, p[:, ::-1]])).reshape(2, 2 * n_deg, n_lon)

    return pack(fwd), pack(c_m * fwd)


def cast_kernel(s_ref, *refs):
    n = len(refs) // 2
    for t in range(n):
        refs[n + t][...] = refs[t][0, 0, 0].astype(BF)


def fwd_dft_kernel(s_ref, tab_ref, *refs):
    pieces, (out, scr, rc) = refs[:8], refs[-3:]
    r = s_ref[2]
    rows = pieces[0].shape[1]
    cols = pieces[0].shape[2]
    nms, nb = out.shape[0], out.shape[1]

    def body(c2, carry):
        for u in range(2):
            c = c2 * 2 + u
            for t in range(8):
                row = pl.multiple_of(((t & 3) ^ r) * rows, rows)
                q = t >> 2
                rc[u, pl.ds(row, rows), q * cols:(q + 1) * cols] = pieces[t][c]
        for u in range(2):
            c = c2 * 2 + u
            res = lax.dot_general(tab_ref[0], rc[u], NT, preferred_element_type=F32)
            for j in range(res.shape[1] // 128):
                scr[j, pl.ds(c, nms, stride=nb + 1), :] = res[:, j * 128:(j + 1) * 128]
        return carry

    lax.fori_loop(0, nb // 2, body, 0)

    def flush(i, carry):
        for j in range(scr.shape[0]):
            for u in range(32):
                out[i * 32 + u, :, j * 128:(j + 1) * 128] = scr[j, pl.ds((i * 32 + u) * (nb + 1), nb), :].astype(BF)
        return carry

    lax.fori_loop(0, nms // 32, flush, 0)


def fwd_leg_kernel(nf, s_ref, *refs):
    pws, fs = refs[:NV], refs[NV:NV + nf]
    mine, send = refs[-2 * NV:-NV], refs[-NV:]
    h = s_ref[3]
    gran = pl.program_id(0) // (MG // MB)
    nl = pws[0].shape[2]
    for g in range(NV):
        @pl.when(gran == g)
        def _(g=g):
            def body(m8, carry):
                for u in range(8):
                    m = m8 * 8 + u
                    x = jnp.concatenate([f[2 * m + s] for s in range(2) for f in fs], axis=0)
                    p = jnp.concatenate([pws[v][m, h] for v in range(g, NV)] + [pws[v][m, 1 - h] for v in range(g, NV)], axis=0)
                    res = lax.dot_general(p, x, NT, preferred_element_type=F32).astype(BF)
                    for v in range(g, NV):
                        for b in range(nl // LB):
                            at = (v - g) * nl + b * LB
                            mine[v][b, m] = res[at:at + LB]
                            at += (NV - g) * nl
                            send[v][b, m] = res[at:at + LB]
                return carry

            lax.fori_loop(0, MB // 8, body, 0)


def mix_kernel(vs, s_ref, wre, wim, *refs):
    ins = {v: refs[4 * n:4 * n + 4] for n, v in enumerate(vs)}
    outs = {v: refs[4 * len(vs) + 2 * n:4 * len(vs) + 2 * n + 2] for n, v in enumerate(vs)}
    scr_a, scr_b = refs[-2:]
    h = s_ref[3]
    for n, v in enumerate(vs):
        @pl.when(pl.program_id(0) // 2 == n)
        def _(v=v):
            nm = MG * (v + 1)

            def fill(i, carry):
                for u in range(16):
                    rows = pl.ds((i * 16 + u) * PAD, LB)
                    for half in range(2):
                        scr_a[2 * half + h, rows, :] = ins[v][half][0, i * 16 + u].astype(F32)
                        scr_a[2 * half + 1 - h, rows, :] = ins[v][2 + half][0, i * 16 + u].astype(F32)
                return carry

            lax.fori_loop(0, nm // 16, fill, 0)

            def body(li2, carry):
                for u in range(2):
                    li = li2 * 2 + u
                    lhs = jnp.concatenate([scr_a[b, pl.ds(li, nm, stride=PAD), :].astype(BF) for b in range(4)], axis=1)
                    wr, wi = wre[li], wim[li]
                    ni = -wi
                    cg = wr.shape[0] // 4
                    rhs = jnp.concatenate([jnp.concatenate([w[b * cg:(b + 1) * cg] for b in range(4) for w in pair], axis=0)
                                           for pair in ((wr, ni), (wi, wr))], axis=1)
                    res = jnp.dot(lhs, rhs, preferred_element_type=F32)
                    for b in range(2):
                        scr_b[b, pl.ds(li, nm, stride=PAD), :] = res[:, b * 128:(b + 1) * 128]
                return carry

            lax.fori_loop(0, LB // 2, body, 0)
            low = lax.broadcasted_iota(jnp.int32, (LB, 128), 1) < 64
            first_is_mine = h == 0

            def flush(i, carry):
                for u in range(16):
                    rows = pl.ds((i * 16 + u) * PAD, LB)
                    re, im = scr_b[0, rows, :], scr_b[1, rows, :]
                    zero = jnp.where(low, re, pltpu.roll(im, 64, 1))
                    one = jnp.where(low, pltpu.roll(re, 64, 1), im)
                    outs[v][0][0, i * 16 + u] = jnp.where(first_is_mine, zero, one).astype(BF)
                    outs[v][1][0, i * 16 + u] = jnp.where(first_is_mine, one, zero).astype(BF)
                return carry

            lax.fori_loop(0, nm // 16, flush, 0)


def inv_leg_kernel(offs, s_ref, *refs):
    pis, bm, br = refs[:NV], refs[NV:2 * NV], refs[2 * NV:3 * NV]
    outs = refs[-len(offs):]
    h = s_ref[3]
    gran = pl.program_id(0) // (MG // MB)
    for g in range(NV):
        @pl.when(gran == g)
        def _(g=g):
            def body(m8, carry):
                for u in range(8):
                    m = m8 * 8 + u
                    b = jnp.concatenate([x[v][lb, m] for x in (bm, br) for v in range(g, NV) for lb in range(2)], axis=0)
                    p = jnp.concatenate([pis[v][m, h] for v in range(g, NV)] + [pis[v][m, 1 - h] for v in range(g, NV)], axis=0)
                    y = lax.dot_general(b, p, TN, preferred_element_type=F32).astype(BF)
                    for o, off in zip(outs, offs):
                        n = o.shape[1]
                        for s in range(2):
                            o[2 * m + s] = y[s * 64 + off:s * 64 + off + n]
                return carry

            lax.fori_loop(0, MB // 8, body, 0)


def inv_dft_kernel(s_ref, tab_ref, g_ref, *refs):
    pieces, (scr, yc) = refs[-10:-2], refs[-2:]
    r = s_ref[2]
    rows = pieces[0].shape[1]
    cols = pieces[0].shape[2]
    nms, nb = g_ref.shape[0], g_ref.shape[1]

    def fill(i, carry):
        for j in range(scr.shape[0]):
            for u in range(32):
                scr[j, pl.ds((i * 32 + u) * (nb + 1), nb), :] = g_ref[i * 32 + u, :, j * 128:(j + 1) * 128].astype(F32)
        return carry

    lax.fori_loop(0, nms // 32, fill, 0)

    def body(c2, carry):
        for u in range(2):
            c = c2 * 2 + u
            g = jnp.concatenate([scr[j, pl.ds(c, nms, stride=nb + 1), :].astype(BF) for j in range(scr.shape[0])], axis=1)
            yc[u] = lax.dot_general(g, tab_ref[0], TN, preferred_element_type=F32).astype(BF)
        for u in range(2):
            c = c2 * 2 + u
            for t in range(8):
                row = pl.multiple_of(((t & 3) ^ r) * rows, rows)
                q = t >> 2
                pieces[t][c] = yc[u, pl.ds(row, rows), q * cols:(q + 1) * cols]
        return carry

    lax.fori_loop(0, nb // 2, body, 0)


def gelu(y):
    return 0.5 * y * (1.0 + lax.erf(y * math.sqrt(0.5)))


def final_kernel(s_ref, f_ref, *refs):
    pieces, (out, buf) = refs[:8], refs[-2:]
    t = pl.program_id(0)
    for n in range(8):
        @pl.when(t == n)
        def _(n=n):
            buf[...] = pieces[n][...]

    def body(c, carry):
        out[0, 0, 0, c] = f_ref[0, 0, 0, c] + gelu(buf[c].astype(F32))
        return carry

    lax.fori_loop(0, buf.shape[0], body, 0)


def call(kernel, grid, in_specs, out_specs, out_shape, flops, nbytes, scratch=(), deps=(), alias=None):
    fn = pl.pallas_call(
        kernel,
        grid_spec=pltpu.PrefetchScalarGridSpec(
            num_scalar_prefetch=1, grid=grid,
            in_specs=list(in_specs) + [pl.BlockSpec(memory_space=pl.ANY)] * len(deps),
            out_specs=out_specs, scratch_shapes=list(scratch)),
        out_shape=out_shape,
        input_output_aliases=alias or {},
        compiler_params=pltpu.CompilerParams(dimension_semantics=("arbitrary",) * len(grid), vmem_limit_bytes=58 * 2 ** 20),
        cost_estimate=pl.CostEstimate(flops=int(flops), bytes_accessed=int(nbytes), transcendentals=0),
    )
    return lambda *args: fn(*args, *deps)


def solution(mesh):
    lat_devs = mesh.shape['lat']
    lon_devs = mesh.shape['lon']
    nd = lat_devs * lon_devs

    def local_layer(grid_field, mix_weight):
        batch, channels, row_count, col_count = grid_field.shape
        n_lat = row_count * lat_devs
        n_lon = col_count * lon_devs
        n_deg = mix_weight.shape[0]
        half_c = batch * channels // nd
        nms = 2 * n_deg
        lv = n_deg // 2 // NV
        q = lax.axis_index('lon')
        r = lax.axis_index('lat')
        me = q * lat_devs + r
        h = r % 2
        scal = jnp.stack([me, q, r, h]).astype(jnp.int32)
        pw_np, pi_np = legendre_tables(n_lat, n_lon, n_deg)
        tf_np, ti_np = dft_tables(n_lon, n_deg)
        pw, pi = [jnp.asarray(x) for x in pw_np], [jnp.asarray(x) for x in pi_np]
        tf, ti = jnp.asarray(tf_np), jnp.asarray(ti_np)
        f6 = grid_field.reshape(batch, 2, channels // half_c, half_c // 2, row_count, col_count)

        def swap(x, t):
            if t == 0:
                return x
            return lax.ppermute(x, ('lon', 'lat'), [(s, s ^ t) for s in range(nd)])

        def piece(cc):
            return jax.ShapeDtypeStruct((cc, row_count, col_count), BF)

        tab_spec = pl.BlockSpec((1, nms, n_lon), lambda i, s: (s[1], 0, 0))

        def piece_spec(nb):
            return pl.BlockSpec((nb, row_count, col_count), lambda i, s: (i, 0, 0))

        def dft_scratch(nb):
            return [pltpu.VMEM((n_lat // 128, nms * (nb + 1), 128), F32), pltpu.VMEM((2, n_lat, n_lon), BF)]

        def cast_chunk(half, c0, cc):
            cb = 8
            base = c0 // cb
            return call(
                cast_kernel, (cc // cb,),
                [pl.BlockSpec((1, 1, 1, cb, row_count, col_count),
                              functools.partial(lambda t, i, s: ((s[0] ^ t) // 2, half, (s[0] ^ t) % 2, base + i, 0, 0), t)) for t in range(nd)],
                [pl.BlockSpec((cb, row_count, col_count), lambda i, s: (i, 0, 0))] * nd,
                [piece(cc)] * nd, 1e6, nd * cc * row_count * col_count * 6)(scal, *([f6] * nd))

        def dft_chunk(pieces, cc, nb, deps):
            return call(
                fwd_dft_kernel, (cc // nb,),
                [tab_spec] + [piece_spec(nb)] * nd,
                pl.BlockSpec((nms, nb, n_lat), lambda i, s: (0, i, 0)),
                jax.ShapeDtypeStruct((nms, cc, n_lat), BF),
                4.0 * cc * nms * n_lat * n_lon, cc * nms * n_lat * 6, dft_scratch(nb), deps)(scal, tf, *pieces)

        last = [MG // MB * (v + 1) - 1 for v in range(NV)]
        tri_specs = [pl.BlockSpec((MB, 2, lv, n_lat), functools.partial(lambda v, i, s: (jnp.minimum(i, last[v]), 0, 0, 0), v)) for v in range(NV)]
        spec_specs = [pl.BlockSpec((lv // LB, MB, LB, half_c), functools.partial(lambda v, i, s: (0, jnp.minimum(i, last[v]), 0, 0), v)) for v in range(NV)]
        spec_shapes = [jax.ShapeDtypeStruct((lv // LB, MG * (v + 1), LB, half_c), BF) for v in range(NV)]

        def f_spec(cc):
            return pl.BlockSpec((2 * MB, cc, n_lat), lambda i, s: (i, 0, 0))

        def leg_fwd(fs):
            res = call(
                functools.partial(fwd_leg_kernel, len(fs)), (n_deg // MB,),
                tri_specs + [f_spec(f.shape[1]) for f in fs],
                spec_specs * 2, spec_shapes * 2,
                1.3 * n_deg * n_deg * n_lat * half_c, 50e6)(scal, *pw, *fs)
            return res[:NV], res[NV:]

        def leg_inv(offs, ccs, mine, recv):
            return call(
                functools.partial(inv_leg_kernel, offs), (n_deg // MB,),
                tri_specs + spec_specs * 2,
                [f_spec(cc) for cc in ccs],
                [jax.ShapeDtypeStruct((nms, cc, n_lat), BF) for cc in ccs],
                1.3 * n_deg * n_deg * n_lat * half_c, 50e6)(scal, *pi, *mine, *recv)

        sizes = HALVES[0] + HALVES[1]
        starts = [(half, sum(part[:k])) for half, part in enumerate(HALVES) for k in range(len(part))]
        recv = []
        for (half, c0), cc in zip(starts, sizes):
            k = len(recv)
            pieces = cast_chunk(half, c0, cc)
            recv.append([swap(p, t) for t, p in enumerate(pieces)])

        w = mix_weight.reshape(n_deg // (2 * LB), 2, LB, channels, channels, 2)
        w = lax.dynamic_index_in_dim(w, h, axis=1, keepdims=False).reshape(n_deg // 2, channels, channels, 2)
        oh = channels // 2
        w_parts = [[w[:, :, x * oh:(x + 1) * oh, p] for p in range(2)] for x in range(2)]

        a_mine, a_recv, prev = [], [], []
        k = 0
        for half in range(2):
            fs = []
            for cc in HALVES[half]:
                deps = list(prev)
                if k == 1:
                    deps += w_parts[0] + w_parts[1]
                elif k == len(HALVES[0]):
                    deps += [a_mine[0][0]]
                fs.append(dft_chunk(recv[k], cc, 8 if k == len(sizes) - 1 else 16, deps))
                prev = fs[-1:]
                k += 1
            mine, send = leg_fwd(fs)
            a_mine.append(mine)
            got = [None] * NV
            for v in sum(MIX, ()):
                got[v] = swap(send[v], 1)
            a_recv.append(got)

        def mix(vs, out_half):
            jump = [lambda j: jnp.minimum(j, 1), lambda j: jnp.maximum(j - 2, 0)]
            w_spec = pl.BlockSpec((LB, channels, channels // 2), lambda j, s: (jnp.where(j < 2, 2 * vs[0] + j, 2 * vs[-1] + j - 2), 0, 0))
            specs, outs, shapes, args = [], [], [], []
            for n, v in enumerate(vs):
                spec = pl.BlockSpec((1, MG * (v + 1), LB, half_c), functools.partial(lambda n, j, s: (jump[n](j), 0, 0, 0), n))
                specs += [spec] * 4
                outs += [spec] * 2
                shapes += [spec_shapes[v]] * 2
                args += [a_mine[0][v], a_mine[1][v], a_recv[0][v], a_recv[1][v]]
            rows = MG * (vs[0] + 1) * PAD
            return call(
                functools.partial(mix_kernel, vs), (2 * len(vs),), [w_spec, w_spec] + specs, outs, shapes,
                4.0 * 4 * LB * MG * (vs[0] + 1) * channels * channels, 40e6,
                [pltpu.VMEM((4, rows, 128), F32), pltpu.VMEM((2, rows, 128), F32)])(scal, *w_parts[out_half], *args)

        def mix_half(half):
            mine, recv = [None] * NV, [None] * NV
            for vs in MIX:
                res = mix(vs, half)
                for n, v in enumerate(vs):
                    mine[v] = res[2 * n]
                    recv[v] = swap(res[2 * n + 1], 1)
            return mine, recv

        def idft_chunk(g, nb):
            cc = g.shape[1]
            return call(
                inv_dft_kernel, (cc // nb,),
                [tab_spec, pl.BlockSpec((nms, nb, n_lat), lambda i, s: (0, i, 0))],
                [piece_spec(nb)] * nd, [piece(cc)] * nd,
                4.0 * cc * nms * n_lat * n_lon, cc * nms * n_lat * 6, dft_scratch(nb))(scal, ti, g)

        def final_chunk(half, c0, cc, pieces, out):
            cb = 8
            base, nb = c0 // cb, cc // cb
            big = pl.BlockSpec((1, 1, 1, cb, row_count, col_count), lambda t, i, s: ((s[0] ^ t) // 2, half, (s[0] ^ t) % 2, base + i, 0, 0))

            def own(n):
                return pl.BlockSpec((cb, row_count, col_count),
                                    lambda t, i, s: (jnp.where(t == n, i, jnp.where(t < n, 0, nb - 1)), 0, 0))

            deps = [] if out is None else [out]
            return call(
                final_kernel, (nd, nb), [big] + [own(n) for n in range(nd)], big,
                jax.ShapeDtypeStruct(f6.shape, F32), 40 * nd * cc * row_count * col_count, 10 * nd * cc * row_count * col_count,
                [pltpu.VMEM((cb, row_count, col_count), BF)], deps,
                {2 + nd: 0} if deps else None)(scal, f6, *pieces)

        k = 0
        out = None
        for half in range(2):
            b_mine, b_recv = mix_half(half)
            offs = [c0 for hf, c0 in starts if hf == half]
            groups = [[0], list(range(1, len(offs)))] if half == 0 else [list(range(len(offs)))]
            gs = []
            for group in groups:
                gs += leg_inv([offs[x] for x in group], [HALVES[half][x] for x in group], b_mine, b_recv)
            for g in gs:
                cc = g.shape[1]
                pieces = idft_chunk(g, 8 if k == 0 else 16)
                got = [swap(p, t) for t, p in enumerate(pieces)]
                if k < len(sizes) - 1:
                    out = final_chunk(*starts[k], cc, got, out)
                else:
                    for t, p in enumerate(got):
                        at = ((me ^ t) // 2, starts[k][0], (me ^ t) % 2, starts[k][1], 0, 0)
                        src = lax.dynamic_slice(f6, at, (1, 1, 1, cc, row_count, col_count))
                        out = lax.dynamic_update_slice(out, src + gelu(p.astype(F32))[None, None, None], at)
                k += 1
        return out.reshape(grid_field.shape)

    field_spec = P('member', None, 'lat', 'lon')
    return jax.shard_map(local_layer, mesh=mesh, in_specs=(field_spec, P()), out_specs=field_spec, check_vma=False)
```
